32 devices in a mesh: dp: 4 (over y, core), ctx: 8 (over z, x).
Axes of the slice: x: 2, y: 2, z: 4, core: 2. Of those that a mesh axis runs over, the one named last changes fastest.
Arguments:
- text: bfloat16 [4, 2, 128, 2048], P('dp', None, None, 'ctx'), may hold values from -6 to 6
- src: int32 [4], replicated, may hold values from 0 to 3, each once
- lengths: int32 [4, 2], replicated, may hold values from 1 to 128
- kv_weight: bfloat16 [2048, 2, 8192], P('dp', None, 'ctx'), may hold values from -0.125 to 0.125
- queries: bfloat16 [4, 2048, 4096], P('dp', 'ctx'), may hold values from -160 to 160
- grad_out: bfloat16 [4, 2048, 4096], P('dp', 'ctx'), may hold values from -6 to 6
Outputs:
- attended: bfloat16 [4, 2048, 4096], P('dp', 'ctx')
- grad_queries: bfloat16 [4, 2048, 4096], P('dp', 'ctx')
- grad_weight: float32 [2048, 2, 8192], P('dp', None, 'ctx')
The draws below stay inside these ranges and needn't reach their ends.
Inputs may be any that keep to these rules, and one draw needn't show every extreme that they name: `src`: each text sample is used by exactly one latent sample. `lengths`: tokens of an encoder output at or beyond its length are padding.
All inputs are finite; a program needn't handle non-finite values.
Results may differ from the reference program's by a relative error of at most 0.018.
The reference program's roundings to bfloat16 on the way count: a program that leaves them out, or rounds other values in their place, can miss the bound.
Values may be sent and summed in bfloat16 or wider, within the bound.
A program may use at most 128 MiB of HBM per device.

```python
import math
import jax
import jax.numpy as jnp
from jax import lax

HEAD = 128
E = 2048
TT = 128
HD = 4096
SAMPLES = 4
LAT = 2048


def draw_queries(key, part):
    base = jax.random.normal(jax.random.fold_in(key, 11), (SAMPLES, LAT, HD), jnp.float32)
    base = jnp.clip(base, -6.0, 6.0)
    return base.astype(jnp.bfloat16)


def set_ends(values, stream_key, smallest, largest):
    longest = values.shape.index(max(values.shape))
    spots = []
    for shift in (0, 1):
        where = [jax.random.randint(jax.random.fold_in(stream_key, axis), (), 0, length) for axis, length in enumerate(values.shape)]
        where[longest] = (where[longest] + shift) % values.shape[longest]
        spots.append(tuple(where))
    return values.at[spots[0]].set(smallest).at[spots[1]].set(largest)


def steps_of(stream_key, shape, split, smallest, top_value):
    def one(axis_at, blocks):
        heights = jax.random.uniform(jax.random.fold_in(jax.random.fold_in(stream_key, 6), axis_at), (blocks,), jnp.float32, smallest / len(split), top_value / len(split))
        return jnp.repeat(jnp.exp(heights), shape[axis_at] // blocks).reshape((-1,) + (1,) * (len(shape) - axis_at - 1))

    gain = one(*split[0])
    for cut in split[1:]:
        gain = gain * one(*cut)
    return gain


def noise(own_key, shape, scale, reach, pieces=(), kind=jnp.bfloat16):
    entries = scale * jax.random.normal(own_key, shape, jnp.float32)
    if pieces:
        entries = entries * steps_of(own_key, shape, pieces, -0.22, 0.18)
    return jnp.clip(entries, -reach, reach).astype(kind)


def setup_inputs(seed: int = 0) -> dict:
    streams_of = jax.random.split(jax.random.key(seed), 7)
    return {
        "text": noise(streams_of[0], (SAMPLES, 2, TT, E), 1.0, 6.0, ((0, 4), (3, 8))),
        "src": jax.random.permutation(streams_of[1], SAMPLES).astype(jnp.int32),
        "lengths": set_ends(jax.random.randint(streams_of[2], (SAMPLES, 2), 1, TT + 1), jax.random.fold_in(streams_of[2], 1), 1, TT).astype(jnp.int32),
        "kv_weight": noise(streams_of[3], (E, 2, 2 * HD), E ** -0.5, 0.125, ((0, 4), (2, 8))),
        "queries": draw_queries(jax.random.fold_in(streams_of[6], 71), 0),
        "grad_out": noise(streams_of[5], (SAMPLES, LAT, HD), 1.0, 6.0, ((0, 4), (1, 8))),
    }


def attend_one(query, key_value, valid, cotangent):
    length = query.shape[0]
    heads = query.shape[1] // HEAD
    keys = key_value.shape[0] * key_value.shape[1]
    scale = 1.0 / math.sqrt(HEAD)
    paired = key_value.reshape(keys, heads, 2, HEAD).astype(jnp.float32)
    key = paired[:, :, 0]
    value = paired[:, :, 1]
    q_rows = query.reshape(length, heads, HEAD).astype(jnp.float32)
    g_rows = cotangent.reshape(length, heads, HEAD).astype(jnp.float32)
    scores = jnp.einsum('lhd,jhd->hlj', q_rows, key) * scale
    scores = jnp.where(valid[None, None, :], scores, -1e+30)
    top = lax.optimization_barrier(jnp.max(scores, axis=-1, keepdims=True))
    weights = jnp.exp(scores - top)
    probs = weights / lax.optimization_barrier(jnp.sum(weights, axis=-1, keepdims=True))
    probs_low = lax.optimization_barrier(probs.astype(jnp.bfloat16)).astype(jnp.float32)
    attended = jnp.einsum('hlj,jhd->lhd', probs_low, value).reshape(length, heads * HEAD).astype(jnp.bfloat16)
    grad_probs = jnp.einsum('lhd,jhd->hlj', g_rows, value)
    delta = lax.optimization_barrier(jnp.sum(probs * grad_probs, axis=-1, keepdims=True))
    grad_scores = (probs * (grad_probs - delta) * scale).astype(jnp.bfloat16)
    grad_scores = lax.optimization_barrier(grad_scores).astype(jnp.float32)
    grad_queries = jnp.einsum('hlj,jhd->lhd', grad_scores, key).reshape(length, heads * HEAD).astype(jnp.bfloat16)
    grad_key = jnp.einsum('hlj,lhd->jhd', grad_scores, q_rows)
    grad_value = jnp.einsum('hlj,lhd->jhd', probs_low, g_rows)
    grad_kv = jnp.stack([grad_key, grad_value], axis=2).reshape(2, keys // 2, heads * 2 * HEAD)
    return (attended, grad_queries, grad_kv)

def reference(text, src, lengths, kv_weight, queries, grad_out):
    ctx_text = jnp.take(text, src.astype(jnp.int32), axis=0)
    wide_text = ctx_text.astype(jnp.float32)
    kv = jnp.einsum('betf,fec->betc', wide_text, kv_weight.astype(jnp.float32)).astype(jnp.bfloat16)
    chosen = jnp.take(lengths, src.astype(jnp.int32), axis=0)
    positions = jnp.arange(TT, dtype=jnp.int32)
    valid = (positions[None, None, :] < chosen[:, :, None]).reshape(SAMPLES, 2 * TT)

    def one_sample(items):
        return attend_one(items[0], items[1], items[2], items[3])
    attended, grad_queries, grad_kv = lax.map(one_sample, (queries, kv, valid, grad_out))
    grad_low = lax.optimization_barrier(grad_kv.astype(jnp.bfloat16)).astype(jnp.float32)
    grad_weight = jnp.einsum('betf,betc->fec', wide_text, grad_low)
    return (attended, grad_queries, grad_weight)
```

```python
import functools
import math

import jax
import jax.numpy as jnp
from jax import lax
from jax.experimental import pallas as pl
from jax.experimental.pallas import tpu as pltpu
from jax.sharding import PartitionSpec as P

HEAD = 128
PAIR = 2 * HEAD
STEP = 32
MESH = pl.DeviceIdType.MESH
VMEM = pl.BlockSpec(memory_space=pltpu.VMEM)
SMEM = pl.BlockSpec(memory_space=pltpu.SMEM)
ANY = pl.BlockSpec(memory_space=pl.ANY)
DMA = pltpu.SemaphoreType.DMA


def dot(a, b, dims):
    return lax.dot_general(a, b, (dims, ((), ())), preferred_element_type=jnp.float32)


def remote(src, dst, send_sem, recv_sem, target):
    return pltpu.make_async_remote_copy(
        src_ref=src, dst_ref=dst, send_sem=send_sem, recv_sem=recv_sem, device_id=target, device_id_type=MESH
    )


class Place:
    def __init__(self, dp, ctx):
        self.rows, self.planes = dp // 2, ctx // 2
        self.last = self.planes - 1
        self.d, self.c = lax.axis_index("dp"), lax.axis_index("ctx")
        self.row, self.core = self.d // 2, self.d % 2
        self.a, self.b = self.c // 2, self.c % 2
        self.up = {"ctx": self.c + 2}
        self.down = {"ctx": self.c - 2}
        self.side = {"ctx": self.a * 2 + 1 - self.b}
        self.twin = {"dp": self.row * 2 + 1 - self.core}

    def at_row(self, row):
        return {"dp": row * 2 + self.core}

    def greet(self):
        barrier = pltpu.get_barrier_semaphore()

        def hello(target):
            pl.semaphore_signal(barrier, inc=1, device_id=target, device_id_type=MESH)

        hello(self.side)
        hello(self.twin)
        for j in range(self.rows):

            @pl.when(self.row != j)
            def _():
                hello(self.at_row(j))

        @pl.when(self.a < self.last)
        def _():
            hello(self.up)

        @pl.when(self.a > 0)
        def _():
            hello(self.down)

        fixed = 1 + self.rows
        if self.last == 0:
            pl.semaphore_wait(barrier, fixed)
        else:

            @pl.when((self.a > 0) & (self.a < self.last))
            def _():
                pl.semaphore_wait(barrier, fixed + 2)

            @pl.when((self.a == 0) | (self.a == self.last))
            def _():
                pl.semaphore_wait(barrier, fixed + 1)


def text_kernel(dp, ctx, src_ref, own_ref, weight_ref, chosen_ref, rows_ref, other_ref, text,
                own_sem, w_sems, row_send, row_recv, line_send, line_recv, twin_send, twin_recv):
    me = Place(dp, ctx)
    rows, a, b, last = me.rows, me.a, me.b, me.last
    share = ctx // dp
    width = own_ref.shape[2]
    features = share * width
    me.greet()
    weights = remote(weight_ref, other_ref, w_sems.at[0], w_sems.at[1], me.twin)

    def spot(piece, core):
        return pl.ds(pl.multiple_of((piece + core * share) % (2 * share) * width, width), width)

    def block(sample, piece, core):
        return text.at[:, sample, :, spot(piece, core)]

    home = me.c // (2 * share)
    piece = me.c % (2 * share)
    mine = pltpu.make_async_copy(own_ref, block(me.d, piece, me.core), own_sem)

    def to_row(row, sample_row):
        return remote(own_ref, block(sample_row * 2 + me.core, piece, me.core), row_send,
                      row_recv.at[sample_row], me.at_row(row))

    def line(i, side, j, way, target):
        p = i * 2 + side
        where = block(j * 2 + me.core, p, me.core)
        return remote(where, where, line_send.at[p, j, way], line_recv.at[p, j], target)

    def across(p, j):
        return remote(block(j * 2 + me.core, p, me.core), block(j * 2 + me.core, p, 1 - me.core),
                      twin_send.at[p, j], twin_recv.at[p, j], me.twin)

    for row in range(rows):

        @pl.when((home == row) & (me.row != row))
        def _():
            to_row(row, me.row).start()

        @pl.when((home == row) & (me.row == row))
        def _():
            mine.start()

    weights.start()
    first = me.row * share
    high = jnp.where(2 * a >= 2 * first + share, 1, 0)
    for t in range(share):
        i = high * (share - 1 - t) + (1 - high) * t
        plane = first + i
        for j_at in range(rows):
            j = (me.row + j_at) % rows

            @pl.when(a == plane)
            def _():
                if j_at == 0:
                    mine.wait()
                else:
                    to_row(0, j).wait_recv()

            @pl.when(a > plane)
            def _():
                line(i, b, j, 0, me.up).wait_recv()

            @pl.when(a < plane)
            def _():
                line(i, b, j, 1, me.down).wait_recv()

            @pl.when((a >= plane) & (a < last))
            def _():
                line(i, b, j, 0, me.up).start()

            @pl.when((a <= plane) & (a > 0))
            def _():
                line(i, b, j, 1, me.down).start()

            line(i, b, j, 2, me.side).start()
            across(i * 2 + b, j).start()

    for t in range(share):
        i = high * (share - 1 - t) + (1 - high) * t
        for j_at in range(rows):
            j = (me.row + j_at) % rows
            line(i, 1 - b, j, 2, me.side).wait_recv()
            across(i * 2 + 1 - b, j).start()

    for p in range(2 * share):
        for j in range(rows):
            across(p, j).wait_recv()
    for b_at in range(dp):
        for e in range(2):
            rows_ref[e, b_at] = text[e, src_ref[b_at], :, pl.ds(0, features)]
    for j in range(rows):
        for e in range(2):
            chosen_ref[e, j] = text[e, src_ref[j * 2 + me.core]]
    for row in range(rows):

        @pl.when((home == row) & (me.row != row))
        def _():
            to_row(row, me.row).wait_send()

    for p in range(2 * share):
        for j in range(rows):
            across(p, j).wait_send()
    for i in range(share):
        plane = first + i
        for j in range(rows):

            @pl.when((a >= plane) & (a < last))
            def _():
                line(i, b, j, 0, me.up).wait_send()

            @pl.when((a <= plane) & (a > 0))
            def _():
                line(i, b, j, 1, me.down).wait_send()

            line(i, b, j, 2, me.side).wait_send()
    weights.wait()


def gather_text(src, own, weight, dp, ctx):
    tokens, width = own.shape[1:]
    share = ctx // dp
    rows = dp // 2
    kind = own.dtype
    pieces = 2 * share
    return pl.pallas_call(
        functools.partial(text_kernel, dp, ctx),
        in_specs=[SMEM, VMEM, ANY],
        out_specs=[VMEM, VMEM, ANY],
        out_shape=[
            jax.ShapeDtypeStruct((2, rows, tokens, pieces * width), kind),
            jax.ShapeDtypeStruct((2, dp, tokens, share * width), kind),
            jax.ShapeDtypeStruct(weight.shape, weight.dtype),
        ],
        scratch_shapes=[
            pltpu.VMEM((2, dp, tokens, pieces * width), kind),
            DMA,
            DMA((2,)),
            DMA,
            DMA((rows,)),
            DMA((pieces, rows, 3)),
            DMA((pieces, rows)),
            DMA((pieces, rows)),
            DMA((pieces, rows)),
        ],
        compiler_params=pltpu.CompilerParams(collective_id=1, has_side_effects=True, vmem_limit_bytes=16 << 20),
        name="gather_text",
    )(src, own, weight)


def sublayer_kernel(dp, ctx, cut, src_ref, lengths_ref, part_ref, q_any, g_any, out_ref, gq_ref, grads_ref,
                    q_ref, g_ref, sums, kv, gkv, crossed0, risen0, fallen0, going0,
                    risen1, fallen1, going1, crossed1,
                    in_sems, y_send, y_recv, ag_send, ag_recv, x0_send, x0_recv,
                    up0_send, up0_recv, down0_send, down0_recv,
                    up1_send, up1_recv, down1_send, down1_recv, x1_send, x1_recv,
                    dp_send, dp_recv, twin_send):
    me = Place(dp, ctx)
    nrows, a, b, last = me.rows, me.a, me.b, me.last
    planes = me.planes
    rounds = kv.shape[0]
    keys = kv.shape[2]
    tokens = keys // 2
    own = me.c
    load_q = pltpu.make_async_copy(q_any, q_ref, in_sems.at[0])
    load_g = pltpu.make_async_copy(g_any, g_ref, in_sems.at[1])
    load_q.start()
    load_g.start()
    me.greet()
    parts = (pl.ds(0, cut), pl.ds(cut, keys - cut))

    def columns(r):
        return pl.ds(pl.multiple_of(r * PAIR, PAIR), PAIR)

    def partial(r, row, sender):
        return remote(part_ref.at[:, row, :, columns(r)], sums.at[r, sender], y_send.at[r, row],
                      y_recv.at[r, sender], me.at_row(row))

    def ag(r, part, block, way, target):
        where = kv.at[r, block, parts[part], :]
        return remote(where, where, ag_send.at[r, part, block, way], ag_recv.at[r, part, block], target)

    def ag_wait(r, part, block):
        ag(r, part, block, 2, me.side).wait_recv()

    def send_up(r, part, block):
        @pl.when(a < last)
        def _():
            ag(r, part, block, 0, me.up).start()

    def send_down(r, part, block):
        @pl.when(a > 0)
        def _():
            ag(r, part, block, 1, me.down).start()

    def start_round(r):
        for j in range(nrows):

            @pl.when(me.row != j)
            def _():
                partial(r, j, j).wait_recv()

        for e in range(2):
            total = part_ref[e, me.row, :, columns(r)]
            for j_at in range(1, nrows):
                total = total + sums[r, (me.row + j_at) % nrows, e]
            kv[r, own, e * tokens:(e + 1) * tokens, :] = total.astype(kv.dtype)
        ag(r, 1, own, 2, me.side).start()
        send_up(r, 0, own)
        send_down(r, 0, own)
        ag(r, 0, own, 2, me.side).start()
        send_up(r, 1, own)
        send_down(r, 1, own)

    def relay_side(r):
        block = a * 2 + 1 - b
        ag_wait(r, 1, block)
        send_up(r, 1, block)
        send_down(r, 1, block)

    def relay(r, s):
        @pl.when(a >= s)
        def _():
            base = (a - s) * 2
            ag_wait(r, 0, base + b)
            send_up(r, 0, base + b)
            ag(r, 0, base + b, 2, me.side).start()
            for side in range(2):
                ag_wait(r, 1, base + side)
                send_up(r, 1, base + side)

        @pl.when(a + s <= last)
        def _():
            base = (a + s) * 2
            ag_wait(r, 0, base + b)
            send_down(r, 0, base + b)
            ag(r, 0, base + b, 2, me.side).start()
            for side in range(2):
                ag_wait(r, 1, base + side)
                send_down(r, 1, base + side)

    scale = 1.0 / math.sqrt(HEAD)
    position = lax.broadcasted_iota(jnp.int32, (1, keys), 1)
    text_at = src_ref[me.d]
    bound = jnp.where(position < tokens, lengths_ref[text_at, 0], lengths_ref[text_at, 1] + tokens)
    bias = jnp.where(position < bound, 0.0, -1e30).astype(jnp.float32)

    def attend(r, block):
        at = pl.ds(pl.multiple_of((block * rounds + r) * HEAD, HEAD), HEAD)
        q = q_ref[:, at]
        g = g_ref[:, at]
        key = kv[r, block, :, :HEAD]
        value = kv[r, block, :, HEAD:]
        scores = dot(q, key, ((1,), (1,))) * scale + bias
        top = jnp.max(scores, axis=-1, keepdims=True)
        weights = jnp.exp(scores - top)
        probs = weights * (1.0 / jnp.sum(weights, axis=-1, keepdims=True))
        probs_low = probs.astype(jnp.bfloat16)
        out_ref[:, at] = dot(probs_low, value, ((1,), (0,))).astype(jnp.bfloat16)
        grad_probs = dot(g, value, ((1,), (1,)))
        delta = jnp.sum(probs * grad_probs, axis=-1, keepdims=True)
        grad_scores = (probs * (grad_probs - delta) * scale).astype(jnp.bfloat16)
        gq_ref[:, at] = dot(grad_scores, key, ((1,), (0,))).astype(jnp.bfloat16)
        gkv[r, block, :, :HEAD] = dot(grad_scores, q, ((0,), (0,))).astype(gkv.dtype)
        gkv[r, block, :, HEAD:] = dot(probs_low, g, ((0,), (0,))).astype(gkv.dtype)

    def cross0(r, z):
        return remote(gkv.at[r, z * 2 + 1 - b, parts[0], :], crossed0.at[r, z], x0_send.at[r, z],
                      x0_recv.at[r, z], me.side)

    def work(r, s):
        @pl.loop(0, 4)
        def _(t):
            way, foreign = t // 2, t % 2
            far = s - foreign
            z = a + far * (2 * way - 1)
            block = z * 2 + b + foreign * (1 - 2 * b)

            @pl.when((z >= 0) & (z <= last) & (far >= 0) & (far <= last) & ((far > 0) | (way == 0)))
            def _():
                @pl.when(foreign == 1)
                def _():
                    ag_wait(r, 0, block)

                attend(r, block)

                @pl.when(foreign == 1)
                def _():
                    cross0(r, z).start()

    def chain0(r, z, rising):
        if rising:
            return remote(going0.at[r, z], risen0.at[r, z], up0_send.at[r, z], up0_recv.at[r, z], me.up)
        return remote(going0.at[r, z], fallen0.at[r, z], down0_send.at[r, z], down0_recv.at[r, z], me.down)

    def chain1(r, z, side, rising, source):
        if rising:
            return remote(source, risen1.at[r, z, side], up1_send.at[r, z, side], up1_recv.at[r, z, side], me.up)
        return remote(source, fallen1.at[r, z, side], down1_send.at[r, z, side], down1_recv.at[r, z, side], me.down)

    def add(target, terms):
        @pl.loop(0, target.shape[0] // STEP)
        def _(i):
            at = pl.ds(pl.multiple_of(i * STEP, STEP), STEP)
            total = terms[0][at, :].astype(jnp.float32)
            for term in terms[1:]:
                total = total + term[at, :].astype(jnp.float32)
            target[at, :] = total.astype(target.dtype)

    def pass_on(r, z, rising, begins):
        arrived0 = risen0 if rising else fallen0
        arrived1 = risen1 if rising else fallen1
        for side in range(2):
            source = gkv.at[r, z * 2 + side, parts[1], :]
            if not begins:
                target = going1.at[r, z, side]
                chain1(r, z, side, rising, target).wait_recv()
                add(target, [source, arrived1.at[r, z, side]])
                source = target
            chain1(r, z, side, rising, source).start()
        cross0(r, z).wait_recv()
        terms = [gkv.at[r, z * 2 + b, parts[0], :], crossed0.at[r, z]]
        if not begins:
            chain0(r, z, rising).wait_recv()
            terms.append(arrived0.at[r, z])
        add(going0.at[r, z], terms)
        chain0(r, z, rising).start()

    def reduce_step(r, s):
        @pl.when(a == s)
        def _():
            for z in range(last, s, -1):
                pass_on(r, z, True, s == 0)

        @pl.when(a == last - s)
        def _():
            for z in range(0, last - s):
                pass_on(r, z, False, s == 0)

    def own_terms(r, low, high, side=None):
        terms = []
        if side is None:
            terms += [risen0.at[r, a]] * low + [fallen0.at[r, a]] * high
        else:
            terms += [risen1.at[r, a, side]] * low + [fallen1.at[r, a, side]] * high
        return terms

    def cross1(r):
        return remote(going1.at[r, a, 1 - b], crossed1.at[r], x1_send.at[r], x1_recv.at[r], me.side)

    def by_place(body):
        @pl.when(a == 0)
        def _():
            body(0, 1)

        @pl.when(a == last)
        def _():
            body(1, 0)

        @pl.when((a > 0) & (a < last))
        def _():
            body(1, 1)

    def finish(r):
        def body(low, high):
            for rising in (True,) * low + (False,) * high:
                for side in range(2):
                    chain1(r, a, side, rising, going1.at[r, a, side]).wait_recv()
            add(going1.at[r, a, 1 - b],
                [gkv.at[r, a * 2 + 1 - b, parts[1], :]] + own_terms(r, low, high, 1 - b))
            cross1(r).start()
            for rising in (True,) * low + (False,) * high:
                chain0(r, a, rising).wait_recv()
            cross0(r, a).wait_recv()
            add(grads_ref.at[me.d, parts[0], columns(r)],
                [gkv.at[r, own, parts[0], :], crossed0.at[r, a]] + own_terms(r, low, high))

        by_place(body)

    def share_grads(r, d, way, target):
        where = grads_ref.at[d, :, columns(r)]
        return remote(where, where, dp_send.at[r, way], dp_recv.at[r, d], target)

    def hand_over(r, d):
        where = grads_ref.at[d, :, columns(r)]
        return remote(where, where, twin_send.at[r, d // 2], dp_recv.at[r, d], me.twin)

    def close(r):
        cross1(r).wait_recv()

        def body(low, high):
            add(grads_ref.at[me.d, parts[1], columns(r)],
                [gkv.at[r, own, parts[1], :], crossed1.at[r]] + own_terms(r, low, high, b))

        by_place(body)
        for j in range(nrows):

            @pl.when(me.row != j)
            def _():
                share_grads(r, me.d, j, me.at_row(j)).start()

        hand_over(r, me.d).start()

    def spread(r):
        for j in range(nrows):

            @pl.when(me.row != j)
            def _():
                d = j * 2 + me.core
                share_grads(r, d, j, me.at_row(j)).wait_recv()
                hand_over(r, d).start()

    @pl.loop(0, rounds)
    def _(r):
        for j in range(nrows):

            @pl.when(me.row != j)
            def _():
                partial(r, j, me.row).start()

    start_round(0)
    load_q.wait()
    load_g.wait()

    @pl.loop(0, rounds + 1)
    def _(i):
        for s in range(planes):

            @pl.when(i > 0)
            def _():
                reduce_step(i - 1, s)

            @pl.when(i < rounds)
            def _():
                if s == 0:
                    relay_side(i)
                else:
                    relay(i, s)
                if s == last:

                    @pl.when(i + 1 < rounds)
                    def _():
                        start_round(i + 1)

                work(i, s)

        @pl.when(i > 1)
        def _():
            close(i - 2)

        @pl.when(i > 0)
        def _():
            finish(i - 1)

        @pl.when(i < rounds)
        def _():
            work(i, planes)

        @pl.when(i > 2)
        def _():
            spread(i - 3)

    close(rounds - 1)
    for r in range(max(rounds - 2, 0), rounds):
        spread(r)

    @pl.loop(0, rounds)
    def _(r):
        for j in range(nrows):
            hand_over(r, j * 2 + 1 - me.core).wait_recv()
            hand_over(r, j * 2 + me.core).wait_send()

            @pl.when(me.row != j)
            def _():
                partial(r, j, me.row).wait_send()
                share_grads(r, me.d, j, me.at_row(j)).wait_send()

        ag(r, 1, own, 2, me.side).wait_send()
        cross1(r).wait_send()
        for z in range(planes):
            cross0(r, z).wait_send()
            ag(r, 0, z * 2 + b, 2, me.side).wait_send()

            @pl.when((a < last) & (z <= a))
            def _():
                ag(r, 0, z * 2 + b, 0, me.up).wait_send()
                for side in range(2):
                    ag(r, 1, z * 2 + side, 0, me.up).wait_send()

            @pl.when((a > 0) & (z >= a))
            def _():
                ag(r, 0, z * 2 + b, 1, me.down).wait_send()
                for side in range(2):
                    ag(r, 1, z * 2 + side, 1, me.down).wait_send()

            for rising in (True, False):

                @pl.when((z > a) if rising else (z < a))
                def _():
                    chain0(r, z, rising).wait_send()
                    for side in range(2):
                        chain1(r, z, side, rising, going1.at[r, z, side]).wait_send()


def sublayer(src, lengths, part, queries, grad_out, dp, ctx):
    _, rows, tokens, columns = part.shape
    rounds = columns // PAIR
    keys = 2 * tokens
    planes = ctx // 2
    cut = keys * 5 // 8 // STEP * STEP
    low = jnp.bfloat16
    first = pltpu.VMEM((rounds, planes, cut, PAIR), low)
    second = pltpu.VMEM((rounds, planes, 2, keys - cut, PAIR), low)
    whole = pltpu.VMEM((rounds, ctx, keys, PAIR), low)
    return pl.pallas_call(
        functools.partial(sublayer_kernel, dp, ctx, cut),
        in_specs=[SMEM, SMEM, VMEM, ANY, ANY],
        out_specs=[VMEM, VMEM, VMEM],
        out_shape=[
            jax.ShapeDtypeStruct(queries.shape, low),
            jax.ShapeDtypeStruct(queries.shape, low),
            jax.ShapeDtypeStruct((dp, keys, columns), low),
        ],
        scratch_shapes=[
            pltpu.VMEM(queries.shape, low),
            pltpu.VMEM(queries.shape, low),
            pltpu.VMEM((rounds, rows, 2, tokens, PAIR), jnp.float32),
            whole,
            whole,
            first,
            first,
            first,
            first,
            second,
            second,
            second,
            pltpu.VMEM((rounds, keys - cut, PAIR), low),
            DMA((2,)),
            DMA((rounds, rows)),
            DMA((rounds, rows)),
            DMA((rounds, 2, ctx, 3)),
            DMA((rounds, 2, ctx)),
        ]
        + [DMA((rounds, planes))] * 6
        + [DMA((rounds, planes, 2))] * 4
        + [
            DMA((rounds,)),
            DMA((rounds,)),
            DMA((rounds, rows)),
            DMA((rounds, dp)),
            DMA((rounds, rows)),
        ],
        compiler_params=pltpu.CompilerParams(collective_id=2, has_side_effects=True, vmem_limit_bytes=50 << 20),
        name="sublayer",
    )(src, lengths, part, queries, grad_out)


def weight_kernel(rows_ref, grads_ref, att_ref, gq_ref, out_ref, att_out, gq_out, buffer, sems):
    keep_att = pltpu.make_async_copy(att_ref, att_out, sems.at[0])
    keep_gq = pltpu.make_async_copy(gq_ref, gq_out, sems.at[1])
    keep_att.start()
    keep_gq.start()
    dp, keys, columns = grads_ref.shape
    tokens = keys // 2
    features = rows_ref.shape[3]
    lanes = columns // HEAD
    stride = 2 * lanes
    size = HEAD

    def ship(i):
        at = pl.ds(i * size * stride, size * stride)
        return pltpu.make_async_copy(buffer.at[at, :], out_ref.at[at, :], sems.at[2 + i])

    for i in range(features // size):
        for e in range(2):
            left = rows_ref[e, :, :, i * size:(i + 1) * size].reshape(dp * tokens, size)
            for j in range(columns // PAIR):
                right = grads_ref[:, e * tokens:(e + 1) * tokens, j * PAIR:(j + 1) * PAIR].reshape(dp * tokens, PAIR)
                block = dot(left, right, ((0,), (0,)))
                for half in range(2):
                    buffer[pl.ds(i * size * stride + (2 * j + half) * 2 + e, size, stride), :] = (
                        block[:, half * HEAD:(half + 1) * HEAD]
                    )
        ship(i).start()
    for i in range(features // size):
        ship(i).wait()
    keep_att.wait()
    keep_gq.wait()


def finish_weight(rows, grads, attended, grad_queries):
    dp, keys, columns = grads.shape
    features = rows.shape[3]
    lanes = columns // HEAD
    flat = (features * lanes * 2, HEAD)
    weight, attended, grad_queries = pl.pallas_call(
        weight_kernel,
        in_specs=[VMEM, VMEM, VMEM, VMEM],
        out_specs=[ANY, ANY, ANY],
        out_shape=[
            jax.ShapeDtypeStruct(flat, jnp.float32),
            jax.ShapeDtypeStruct(attended.shape, attended.dtype),
            jax.ShapeDtypeStruct(attended.shape, attended.dtype),
        ],
        scratch_shapes=[pltpu.VMEM(flat, jnp.float32), DMA((2 + features // HEAD,))],
        compiler_params=pltpu.CompilerParams(vmem_limit_bytes=24 << 20),
        name="finish_weight",
    )(rows, grads, attended, grad_queries)
    weight = weight.reshape(features, lanes, 2, HEAD).transpose(0, 2, 1, 3).reshape(features, 2, columns)
    return attended, grad_queries, weight


def per_device(dp, ctx, text, src, lengths, kv_weight, queries, grad_out):
    features = kv_weight.shape[0]
    chosen, rows, other = gather_text(src, text[0], kv_weight, dp, ctx)
    dims = "ejtf,fec->ejtc"
    part = jnp.einsum(dims, chosen[..., :features], kv_weight, preferred_element_type=jnp.float32)
    part = part + jnp.einsum(dims, chosen[..., features:], other, preferred_element_type=jnp.float32)
    attended, grad_queries, grads = sublayer(src, lengths, part, queries[0], grad_out[0], dp, ctx)
    attended, grad_queries, weight = finish_weight(rows, grads, attended, grad_queries)
    return (attended[None], grad_queries[None], weight)


def solution(mesh):
    placed = (
        P("dp", None, None, "ctx"),
        P(),
        P(),
        P("dp", None, "ctx"),
        P("dp", "ctx", None),
        P("dp", "ctx", None),
    )
    return jax.shard_map(
        functools.partial(per_device, mesh.shape["dp"], mesh.shape["ctx"]),
        mesh=mesh,
        in_specs=placed,
        out_specs=(P("dp", "ctx", None), P("dp", "ctx", None), P("dp", None, "ctx")),
        check_vma=False,
    )
```

```python
import functools
import math

import jax
import jax.numpy as jnp
from jax import lax
from jax.experimental import pallas as pl
from jax.experimental.pallas import tpu as pltpu
from jax.sharding import PartitionSpec as P

HEAD = 128
PAIR = 2 * HEAD
STEP = 32
MESH = pl.DeviceIdType.MESH
VMEM = pl.BlockSpec(memory_space=pltpu.VMEM)
SMEM = pl.BlockSpec(memory_space=pltpu.SMEM)
ANY = pl.BlockSpec(memory_space=pl.ANY)
HBM = pl.BlockSpec(memory_space=pltpu.HBM)
DMA = pltpu.SemaphoreType.DMA


def dot(a, b, dims):
    return lax.dot_general(a, b, (dims, ((), ())), preferred_element_type=jnp.float32)


def remote(src, dst, send_sem, recv_sem, target):
    return pltpu.make_async_remote_copy(
        src_ref=src, dst_ref=dst, send_sem=send_sem, recv_sem=recv_sem, device_id=target, device_id_type=MESH
    )


class Place:
    def __init__(self, dp, ctx):
        self.rows, self.planes = dp // 2, ctx // 2
        self.last = self.planes - 1
        self.d, self.c = lax.axis_index("dp"), lax.axis_index("ctx")
        self.row, self.core = self.d // 2, self.d % 2
        self.a, self.b = self.c // 2, self.c % 2
        self.up = {"ctx": self.c + 2}
        self.down = {"ctx": self.c - 2}
        self.side = {"ctx": self.a * 2 + 1 - self.b}
        self.twin = {"dp": self.row * 2 + 1 - self.core}

    def at_row(self, row):
        return {"dp": row * 2 + self.core}

    def greet(self):
        barrier = pltpu.get_barrier_semaphore()

        def hello(target):
            pl.semaphore_signal(barrier, inc=1, device_id=target, device_id_type=MESH)

        hello(self.side)
        hello(self.twin)
        for j in range(self.rows):

            @pl.when(self.row != j)
            def _():
                hello(self.at_row(j))

        @pl.when(self.a < self.last)
        def _():
            hello(self.up)

        @pl.when(self.a > 0)
        def _():
            hello(self.down)

        fixed = 1 + self.rows
        if self.last == 0:
            pl.semaphore_wait(barrier, fixed)
        else:

            @pl.when((self.a > 0) & (self.a < self.last))
            def _():
                pl.semaphore_wait(barrier, fixed + 2)

            @pl.when((self.a == 0) | (self.a == self.last))
            def _():
                pl.semaphore_wait(barrier, fixed + 1)


def text_kernel(dp, ctx, src_any, own_ref, weight_ref, chosen_ref, rows_ref, pair_ref, src_ref, text,
                own_sem, src_sem, w_sems, row_send, row_recv, line_send, line_recv, twin_send, twin_recv):
    me = Place(dp, ctx)
    rows, a, b, last = me.rows, me.a, me.b, me.last
    share = ctx // dp
    width = own_ref.shape[2]
    features = share * width
    load_src = pltpu.make_async_copy(src_any, src_ref, src_sem)
    load_src.start()
    weights = remote(weight_ref, pair_ref.at[1], w_sems.at[0], w_sems.at[1], me.twin)
    own_weights = pltpu.make_async_copy(weight_ref, pair_ref.at[0], w_sems.at[2])
    own_weights.start()
    me.greet()

    def spot(piece, core):
        return pl.ds(pl.multiple_of((piece + core * share) % (2 * share) * width, width), width)

    def block(sample, piece, core):
        return text.at[:, sample, :, spot(piece, core)]

    home = me.c // (2 * share)
    piece = me.c % (2 * share)
    mine = pltpu.make_async_copy(own_ref, block(me.d, piece, me.core), own_sem)

    def to_row(row, sample_row):
        return remote(own_ref, block(sample_row * 2 + me.core, piece, me.core), row_send,
                      row_recv.at[sample_row], me.at_row(row))

    def line(i, side, j, way, target):
        p = i * 2 + side
        where = block(j * 2 + me.core, p, me.core)
        return remote(where, where, line_send.at[p, j, way], line_recv.at[p, j], target)

    def across(p, j):
        return remote(block(j * 2 + me.core, p, me.core), block(j * 2 + me.core, p, 1 - me.core),
                      twin_send.at[p, j], twin_recv.at[p, j], me.twin)

    for row in range(rows):

        @pl.when((home == row) & (me.row != row))
        def _():
            to_row(row, me.row).start()

        @pl.when((home == row) & (me.row == row))
        def _():
            mine.start()

    weights.start()
    first = me.row * share
    high = jnp.where(2 * a >= 2 * first + share, 1, 0)
    for t in range(share):
        i = high * (share - 1 - t) + (1 - high) * t
        plane = first + i
        for j_at in range(rows):
            j = (me.row + j_at) % rows

            @pl.when(a == plane)
            def _():
                if j_at == 0:
                    mine.wait()
                else:
                    to_row(0, j).wait_recv()

            @pl.when(a > plane)
            def _():
                line(i, b, j, 0, me.up).wait_recv()

            @pl.when(a < plane)
            def _():
                line(i, b, j, 1, me.down).wait_recv()

            @pl.when((a >= plane) & (a < last))
            def _():
                line(i, b, j, 0, me.up).start()

            @pl.when((a <= plane) & (a > 0))
            def _():
                line(i, b, j, 1, me.down).start()

            line(i, b, j, 2, me.side).start()
            across(i * 2 + b, j).start()

    for t in range(share):
        i = high * (share - 1 - t) + (1 - high) * t
        for j_at in range(rows):
            j = (me.row + j_at) % rows
            line(i, 1 - b, j, 2, me.side).wait_recv()
            across(i * 2 + 1 - b, j).start()

    for p in range(2 * share):
        for j in range(rows):
            across(p, j).wait_recv()
    load_src.wait()
    for b_at in range(dp):
        for e in range(2):
            rows_ref[e, b_at] = text[e, src_ref[b_at], :, pl.ds(0, features)]
    for j in range(rows):
        for e in range(2):
            chosen_ref[e, j] = text[e, src_ref[j * 2 + me.core]]
    for row in range(rows):

        @pl.when((home == row) & (me.row != row))
        def _():
            to_row(row, me.row).wait_send()

    for p in range(2 * share):
        for j in range(rows):
            across(p, j).wait_send()
    for i in range(share):
        plane = first + i
        for j in range(rows):

            @pl.when((a >= plane) & (a < last))
            def _():
                line(i, b, j, 0, me.up).wait_send()

            @pl.when((a <= plane) & (a > 0))
            def _():
                line(i, b, j, 1, me.down).wait_send()

            line(i, b, j, 2, me.side).wait_send()
    weights.wait()
    own_weights.wait()


def gather_text(src, own, weight, dp, ctx):
    tokens, width = own.shape[1:]
    share = ctx // dp
    rows = dp // 2
    kind = own.dtype
    pieces = 2 * share
    return pl.pallas_call(
        functools.partial(text_kernel, dp, ctx),
        in_specs=[HBM, HBM, HBM],
        out_specs=[VMEM, VMEM, VMEM],
        out_shape=[
            jax.ShapeDtypeStruct((2, rows, tokens, pieces * width), kind),
            jax.ShapeDtypeStruct((2, dp, tokens, share * width), kind),
            jax.ShapeDtypeStruct((2,) + weight.shape, weight.dtype),
        ],
        scratch_shapes=[
            pltpu.SMEM(src.shape, src.dtype),
            pltpu.VMEM((2, dp, tokens, pieces * width), kind),
            DMA,
            DMA,
            DMA((3,)),
            DMA,
            DMA((rows,)),
            DMA((pieces, rows, 3)),
            DMA((pieces, rows)),
            DMA((pieces, rows)),
            DMA((pieces, rows)),
        ],
        compiler_params=pltpu.CompilerParams(collective_id=1, has_side_effects=True, vmem_limit_bytes=16 << 20),
        name="gather_text",
    )(src, own, weight)


def sublayer_kernel(dp, ctx, cut, src_any, lengths_any, part_ref, q_any, g_any, out_ref, gq_ref, grads_ref,
                    src_ref, lengths_ref, q_ref, g_ref, sums, kv, gkv, crossed0, risen0, fallen0, going0,
                    risen1, fallen1, going1, crossed1,
                    in_sems, y_send, y_recv, ag_send, ag_recv, x0_send, x0_recv,
                    up0_send, up0_recv, down0_send, down0_recv,
                    up1_send, up1_recv, down1_send, down1_recv, x1_send, x1_recv,
                    dp_send, dp_recv, twin_send):
    me = Place(dp, ctx)
    nrows, a, b, last = me.rows, me.a, me.b, me.last
    planes = me.planes
    rounds = kv.shape[0]
    keys = kv.shape[2]
    tokens = keys // 2
    own = me.c
    load_q = pltpu.make_async_copy(q_any, q_ref, in_sems.at[0])
    load_g = pltpu.make_async_copy(g_any, g_ref, in_sems.at[1])
    load_src = pltpu.make_async_copy(src_any, src_ref, in_sems.at[2])
    load_lengths = pltpu.make_async_copy(lengths_any, lengths_ref, in_sems.at[3])
    load_src.start()
    load_lengths.start()
    load_q.start()
    load_g.start()
    me.greet()
    parts = (pl.ds(0, cut), pl.ds(cut, keys - cut))

    def columns(r):
        return pl.ds(pl.multiple_of(r * PAIR, PAIR), PAIR)

    def partial(r, row, sender):
        return remote(part_ref.at[:, row, :, columns(r)], sums.at[r, sender], y_send.at[r, row],
                      y_recv.at[r, sender], me.at_row(row))

    def ag(r, part, block, way, target):
        where = kv.at[r, block, parts[part], :]
        return remote(where, where, ag_send.at[r, part, block, way], ag_recv.at[r, part, block], target)

    def ag_wait(r, part, block):
        ag(r, part, block, 2, me.side).wait_recv()

    def send_up(r, part, block):
        @pl.when(a < last)
        def _():
            ag(r, part, block, 0, me.up).start()

    def send_down(r, part, block):
        @pl.when(a > 0)
        def _():
            ag(r, part, block, 1, me.down).start()

    def start_round(r):
        for j in range(nrows):

            @pl.when(me.row != j)
            def _():
                partial(r, j, j).wait_recv()

        for e in range(2):
            total = part_ref[e, me.row, :, columns(r)]
            for j_at in range(1, nrows):
                total = total + sums[r, (me.row + j_at) % nrows, e]
            kv[r, own, e * tokens:(e + 1) * tokens, :] = total.astype(kv.dtype)
        ag(r, 1, own, 2, me.side).start()
        send_up(r, 0, own)
        send_down(r, 0, own)
        ag(r, 0, own, 2, me.side).start()
        send_up(r, 1, own)
        send_down(r, 1, own)

    def relay_side(r):
        block = a * 2 + 1 - b
        ag_wait(r, 1, block)
        send_up(r, 1, block)
        send_down(r, 1, block)

    def relay(r, s):
        @pl.when(a >= s)
        def _():
            base = (a - s) * 2
            ag_wait(r, 0, base + b)
            send_up(r, 0, base + b)
            ag(r, 0, base + b, 2, me.side).start()
            for side in range(2):
                ag_wait(r, 1, base + side)
                send_up(r, 1, base + side)

        @pl.when(a + s <= last)
        def _():
            base = (a + s) * 2
            ag_wait(r, 0, base + b)
            send_down(r, 0, base + b)
            ag(r, 0, base + b, 2, me.side).start()
            for side in range(2):
                ag_wait(r, 1, base + side)
                send_down(r, 1, base + side)

    scale = 1.0 / math.sqrt(HEAD)
    position = lax.broadcasted_iota(jnp.int32, (1, keys), 1)
    load_src.wait()
    load_lengths.wait()
    text_at = src_ref[me.d]
    bound = jnp.where(position < tokens, lengths_ref[0, text_at], lengths_ref[1, text_at] + tokens)
    bias = jnp.where(position < bound, 0.0, -1e30).astype(jnp.float32)

    def attend(r, block):
        at = pl.ds(pl.multiple_of((block * rounds + r) * HEAD, HEAD), HEAD)
        q = q_ref[:, at]
        g = g_ref[:, at]
        key = kv[r, block, :, :HEAD]
        value = kv[r, block, :, HEAD:]
        scores = dot(q, key, ((1,), (1,))) * scale + bias
        grad_probs = dot(g, value, ((1,), (1,)))
        top = jnp.max(scores, axis=-1, keepdims=True)
        weights = jnp.exp(scores - top)
        probs = weights * (1.0 / jnp.sum(weights, axis=-1, keepdims=True))
        probs_low = probs.astype(jnp.bfloat16)
        delta = jnp.sum(probs * grad_probs, axis=-1, keepdims=True)
        grad_scores = (probs * (grad_probs - delta) * scale).astype(jnp.bfloat16)
        out_ref[:, at] = dot(probs_low, value, ((1,), (0,))).astype(jnp.bfloat16)
        gq_ref[:, at] = dot(grad_scores, key, ((1,), (0,))).astype(jnp.bfloat16)
        gkv[r, block, :, :HEAD] = dot(grad_scores, q, ((0,), (0,))).astype(gkv.dtype)
        gkv[r, block, :, HEAD:] = dot(probs_low, g, ((0,), (0,))).astype(gkv.dtype)

    def cross0(r, z):
        return remote(gkv.at[r, z * 2 + 1 - b, parts[0], :], crossed0.at[r, z], x0_send.at[r, z],
                      x0_recv.at[r, z], me.side)

    def work(r, s):
        @pl.loop(0, 4)
        def _(t):
            way, foreign = t // 2, t % 2
            far = s - foreign
            z = a + far * (2 * way - 1)
            block = z * 2 + b + foreign * (1 - 2 * b)

            @pl.when((z >= 0) & (z <= last) & (far >= 0) & (far <= last) & ((far > 0) | (way == 0)))
            def _():
                @pl.when(foreign == 1)
                def _():
                    ag_wait(r, 0, block)

                attend(r, block)

                @pl.when(foreign == 1)
                def _():
                    cross0(r, z).start()

    def chain0(r, z, rising):
        if rising:
            return remote(going0.at[r, z], risen0.at[r, z], up0_send.at[r, z], up0_recv.at[r, z], me.up)
        return remote(going0.at[r, z], fallen0.at[r, z], down0_send.at[r, z], down0_recv.at[r, z], me.down)

    def chain1(r, z, side, rising, source):
        if rising:
            return remote(source, risen1.at[r, z, side], up1_send.at[r, z, side], up1_recv.at[r, z, side], me.up)
        return remote(source, fallen1.at[r, z, side], down1_send.at[r, z, side], down1_recv.at[r, z, side], me.down)

    def add(target, terms):
        @pl.loop(0, target.shape[0] // STEP)
        def _(i):
            at = pl.ds(pl.multiple_of(i * STEP, STEP), STEP)
            total = terms[0][at, :].astype(jnp.float32)
            for term in terms[1:]:
                total = total + term[at, :].astype(jnp.float32)
            target[at, :] = total.astype(target.dtype)

    def pass_on(r, z, rising, begins):
        arrived0 = risen0 if rising else fallen0
        arrived1 = risen1 if rising else fallen1
        for side in range(2):
            source = gkv.at[r, z * 2 + side, parts[1], :]
            if not begins:
                target = going1.at[r, z, side]
                chain1(r, z, side, rising, target).wait_recv()
                add(target, [source, arrived1.at[r, z, side]])
                source = target
            chain1(r, z, side, rising, source).start()
        cross0(r, z).wait_recv()
        terms = [gkv.at[r, z * 2 + b, parts[0], :], crossed0.at[r, z]]
        if not begins:
            chain0(r, z, rising).wait_recv()
            terms.append(arrived0.at[r, z])
        add(going0.at[r, z], terms)
        chain0(r, z, rising).start()

    def reduce_step(r, s):
        @pl.when(a == 0)
        def _():
            pass_on(r, last + 1 - s, True, True)

        @pl.when((a > 0) & (a < s))
        def _():
            pass_on(r, last + a + 1 - s, True, False)

        @pl.when(a == last)
        def _():
            pass_on(r, s - 1, False, True)

        @pl.when((a < last) & (last - a < s))
        def _():
            pass_on(r, s - last + a - 1, False, False)

    def own_terms(r, low, high, side=None):
        terms = []
        if side is None:
            terms += [risen0.at[r, a]] * low + [fallen0.at[r, a]] * high
        else:
            terms += [risen1.at[r, a, side]] * low + [fallen1.at[r, a, side]] * high
        return terms

    def cross1(r):
        return remote(going1.at[r, a, 1 - b], crossed1.at[r], x1_send.at[r], x1_recv.at[r], me.side)

    def by_place(body):
        @pl.when(a == 0)
        def _():
            body(0, 1)

        @pl.when(a == last)
        def _():
            body(1, 0)

        @pl.when((a > 0) & (a < last))
        def _():
            body(1, 1)

    def finish(r):
        def body(low, high):
            for rising in (True,) * low + (False,) * high:
                for side in range(2):
                    chain1(r, a, side, rising, going1.at[r, a, side]).wait_recv()
            add(going1.at[r, a, 1 - b],
                [gkv.at[r, a * 2 + 1 - b, parts[1], :]] + own_terms(r, low, high, 1 - b))
            cross1(r).start()
            for rising in (True,) * low + (False,) * high:
                chain0(r, a, rising).wait_recv()
            cross0(r, a).wait_recv()
            add(grads_ref.at[me.d, parts[0], columns(r)],
                [gkv.at[r, own, parts[0], :], crossed0.at[r, a]] + own_terms(r, low, high))

        by_place(body)

    def share_grads(r, d, way, target):
        where = grads_ref.at[d, :, columns(r)]
        return remote(where, where, dp_send.at[r, way], dp_recv.at[r, d], target)

    def hand_over(r, d):
        where = grads_ref.at[d, :, columns(r)]
        return remote(where, where, twin_send.at[r, d // 2], dp_recv.at[r, d], me.twin)

    def close(r):
        cross1(r).wait_recv()

        def body(low, high):
            add(grads_ref.at[me.d, parts[1], columns(r)],
                [gkv.at[r, own, parts[1], :], crossed1.at[r]] + own_terms(r, low, high, b))

        by_place(body)
        for j in range(nrows):

            @pl.when(me.row != j)
            def _():
                share_grads(r, me.d, j, me.at_row(j)).start()

        hand_over(r, me.d).start()

    def spread(r):
        for j in range(nrows):

            @pl.when(me.row != j)
            def _():
                d = j * 2 + me.core
                share_grads(r, d, j, me.at_row(j)).wait_recv()
                hand_over(r, d).start()

    @pl.loop(0, rounds)
    def _(r):
        for j in range(nrows):

            @pl.when(me.row != j)
            def _():
                partial(r, j, me.row).start()

    start_round(0)
    load_q.wait()
    load_g.wait()

    @pl.loop(0, rounds + 1)
    def _(i):
        for s in range(planes):

            @pl.when(i < rounds)
            def _():
                if s == 0:
                    relay_side(i)
                else:
                    relay(i, s)

            if s > 0:

                @pl.when(i > 0)
                def _():
                    reduce_step(i - 1, s)

            if s == last:

                @pl.when(i + 1 < rounds)
                def _():
                    start_round(i + 1)

            if s == min(1, last):

                @pl.when(i > 1)
                def _():
                    finish(i - 2)

            if s == min(2, last):

                @pl.when(i > 1)
                def _():
                    close(i - 2)

            if s == last:

                @pl.when(i > 2)
                def _():
                    spread(i - 3)

            @pl.when(i < rounds)
            def _():
                work(i, s)

        @pl.when(i < rounds)
        def _():
            work(i, planes)

    finish(rounds - 1)
    close(rounds - 1)
    for r in range(max(rounds - 2, 0), rounds):
        spread(r)

    @pl.loop(0, rounds)
    def _(r):
        for j in range(nrows):
            hand_over(r, j * 2 + 1 - me.core).wait_recv()
            hand_over(r, j * 2 + me.core).wait_send()

            @pl.when(me.row != j)
            def _():
                partial(r, j, me.row).wait_send()
                share_grads(r, me.d, j, me.at_row(j)).wait_send()

        ag(r, 1, own, 2, me.side).wait_send()
        cross1(r).wait_send()
        for z in range(planes):
            cross0(r, z).wait_send()
            ag(r, 0, z * 2 + b, 2, me.side).wait_send()

            @pl.when((a < last) & (z <= a))
            def _():
                ag(r, 0, z * 2 + b, 0, me.up).wait_send()
                for side in range(2):
                    ag(r, 1, z * 2 + side, 0, me.up).wait_send()

            @pl.when((a > 0) & (z >= a))
            def _():
                ag(r, 0, z * 2 + b, 1, me.down).wait_send()
                for side in range(2):
                    ag(r, 1, z * 2 + side, 1, me.down).wait_send()

            for rising in (True, False):

                @pl.when((z > a) if rising else (z < a))
                def _():
                    chain0(r, z, rising).wait_send()
                    for side in range(2):
                        chain1(r, z, side, rising, going1.at[r, z, side]).wait_send()


def sublayer(src, lengths, part, queries, grad_out, dp, ctx):
    _, rows, tokens, columns = part.shape
    rounds = columns // PAIR
    keys = 2 * tokens
    planes = ctx // 2
    cut = keys * 5 // 8 // STEP * STEP
    low = jnp.bfloat16
    first = pltpu.VMEM((rounds, planes, cut, PAIR), low)
    second = pltpu.VMEM((rounds, planes, 2, keys - cut, PAIR), low)
    whole = pltpu.VMEM((rounds, ctx, keys, PAIR), low)
    return pl.pallas_call(
        functools.partial(sublayer_kernel, dp, ctx, cut),
        in_specs=[HBM, HBM, VMEM, HBM, HBM],
        out_specs=[VMEM, VMEM, VMEM],
        out_shape=[
            jax.ShapeDtypeStruct(queries.shape, low),
            jax.ShapeDtypeStruct(queries.shape, low),
            jax.ShapeDtypeStruct((dp, keys, columns), low),
        ],
        scratch_shapes=[
            pltpu.SMEM(src.shape, src.dtype),
            pltpu.SMEM(lengths.shape, lengths.dtype),
            pltpu.VMEM(queries.shape, low),
            pltpu.VMEM(queries.shape, low),
            pltpu.VMEM((rounds, rows, 2, tokens, PAIR), jnp.float32),
            whole,
            whole,
            first,
            first,
            first,
            first,
            second,
            second,
            second,
            pltpu.VMEM((rounds, keys - cut, PAIR), low),
            DMA((4,)),
            DMA((rounds, rows)),
            DMA((rounds, rows)),
            DMA((rounds, 2, ctx, 3)),
            DMA((rounds, 2, ctx)),
        ]
        + [DMA((rounds, planes))] * 6
        + [DMA((rounds, planes, 2))] * 4
        + [
            DMA((rounds,)),
            DMA((rounds,)),
            DMA((rounds, rows)),
            DMA((rounds, dp)),
            DMA((rounds, rows)),
        ],
        compiler_params=pltpu.CompilerParams(collective_id=2, has_side_effects=True, vmem_limit_bytes=36 << 20),
        name="sublayer",
    )(src, lengths, part, queries, grad_out)


def weight_kernel(rows_ref, grads_ref, att_ref, gq_ref, out_ref, att_out, gq_out, buffer, sems):
    keep_att = pltpu.make_async_copy(att_ref, att_out, sems.at[0])
    keep_gq = pltpu.make_async_copy(gq_ref, gq_out, sems.at[1])
    keep_att.start()
    keep_gq.start()
    dp, keys, columns = grads_ref.shape
    tokens = keys // 2
    features = rows_ref.shape[3]
    lanes = columns // HEAD
    stride = 2 * lanes
    size = HEAD

    def ship(i):
        at = pl.ds(i * size * stride, size * stride)
        return pltpu.make_async_copy(buffer.at[at, :], out_ref.at[at, :], sems.at[2 + i])

    for i in range(features // size):
        for e in range(2):
            left = rows_ref[e, :, :, i * size:(i + 1) * size].reshape(dp * tokens, size)
            for j in range(columns // PAIR):
                right = grads_ref[:, e * tokens:(e + 1) * tokens, j * PAIR:(j + 1) * PAIR].reshape(dp * tokens, PAIR)
                block = dot(left, right, ((0,), (0,)))
                for half in range(2):
                    buffer[pl.ds(i * size * stride + (2 * j + half) * 2 + e, size, stride), :] = (
                        block[:, half * HEAD:(half + 1) * HEAD]
                    )
        ship(i).start()
    for i in range(features // size):
        ship(i).wait()
    keep_att.wait()
    keep_gq.wait()


def finish_weight(rows, grads, attended, grad_queries):
    dp, keys, columns = grads.shape
    features = rows.shape[3]
    lanes = columns // HEAD
    flat = (features * lanes * 2, HEAD)
    weight, attended, grad_queries = pl.pallas_call(
        weight_kernel,
        in_specs=[VMEM, VMEM, VMEM, VMEM],
        out_specs=[ANY, ANY, ANY],
        out_shape=[
            jax.ShapeDtypeStruct(flat, jnp.float32),
            jax.ShapeDtypeStruct(attended.shape, attended.dtype),
            jax.ShapeDtypeStruct(attended.shape, attended.dtype),
        ],
        scratch_shapes=[pltpu.VMEM(flat, jnp.float32), DMA((2 + features // HEAD,))],
        compiler_params=pltpu.CompilerParams(vmem_limit_bytes=24 << 20),
        name="finish_weight",
    )(rows, grads, attended, grad_queries)
    weight = weight.reshape(features, lanes, 2, HEAD).transpose(0, 2, 1, 3).reshape(features, 2, columns)
    return attended, grad_queries, weight


def per_device(dp, ctx, text, src, lengths, kv_weight, queries, grad_out):
    chosen, rows, pair = gather_text(src, text[0], kv_weight, dp, ctx)
    dims = "ejtf,fec->ejtc"
    pair = pair.reshape((-1,) + kv_weight.shape[1:])
    part = jnp.einsum(dims, chosen, pair, preferred_element_type=jnp.float32)
    attended, grad_queries, grads = sublayer(src, lengths.T, part, queries[0], grad_out[0], dp, ctx)
    attended, grad_queries, weight = finish_weight(rows, grads, attended, grad_queries)
    return (attended[None], grad_queries[None], weight)


def solution(mesh):
    placed = (
        P("dp", None, None, "ctx"),
        P(),
        P(),
        P("dp", None, "ctx"),
        P("dp", "ctx", None),
        P("dp", "ctx", None),
    )
    return jax.shard_map(
        functools.partial(per_device, mesh.shape["dp"], mesh.shape["ctx"]),
        mesh=mesh,
        in_specs=placed,
        out_specs=(P("dp", "ctx", None), P("dp", "ctx", None), P("dp", None, "ctx")),
        check_vma=False,
    )
```

```python
import functools
import math

import jax
import jax.numpy as jnp
from jax import lax
from jax.experimental import pallas as pl
from jax.experimental.pallas import tpu as pltpu
from jax.sharding import PartitionSpec as P

HEAD = 128
PAIR = 2 * HEAD
STEP = 32
MESH = pl.DeviceIdType.MESH
VMEM = pl.BlockSpec(memory_space=pltpu.VMEM)
SMEM = pl.BlockSpec(memory_space=pltpu.SMEM)
ANY = pl.BlockSpec(memory_space=pl.ANY)
HBM = pl.BlockSpec(memory_space=pltpu.HBM)
DMA = pltpu.SemaphoreType.DMA


def dot(a, b, dims):
    return lax.dot_general(a, b, (dims, ((), ())), preferred_element_type=jnp.float32)


def remote(src, dst, send_sem, recv_sem, target):
    return pltpu.make_async_remote_copy(
        src_ref=src, dst_ref=dst, send_sem=send_sem, recv_sem=recv_sem, device_id=target, device_id_type=MESH
    )


class Place:
    def __init__(self, dp, ctx):
        self.rows, self.planes = dp // 2, ctx // 2
        self.last = self.planes - 1
        self.d, self.c = lax.axis_index("dp"), lax.axis_index("ctx")
        self.row, self.core = self.d // 2, self.d % 2
        self.a, self.b = self.c // 2, self.c % 2
        self.up = {"ctx": self.c + 2}
        self.down = {"ctx": self.c - 2}
        self.side = {"ctx": self.a * 2 + 1 - self.b}
        self.twin = {"dp": self.row * 2 + 1 - self.core}

    def at_row(self, row):
        return {"dp": row * 2 + self.core}

    def greet(self):
        barrier = pltpu.get_barrier_semaphore()

        def hello(target):
            pl.semaphore_signal(barrier, inc=1, device_id=target, device_id_type=MESH)

        hello(self.side)
        hello(self.twin)
        for j in range(self.rows):

            @pl.when(self.row != j)
            def _():
                hello(self.at_row(j))

        @pl.when(self.a < self.last)
        def _():
            hello(self.up)

        @pl.when(self.a > 0)
        def _():
            hello(self.down)

        fixed = 1 + self.rows
        if self.last == 0:
            pl.semaphore_wait(barrier, fixed)
        else:

            @pl.when((self.a > 0) & (self.a < self.last))
            def _():
                pl.semaphore_wait(barrier, fixed + 2)

            @pl.when((self.a == 0) | (self.a == self.last))
            def _():
                pl.semaphore_wait(barrier, fixed + 1)


def text_kernel(dp, ctx, src_any, own_ref, weight_ref, chosen_ref, rows_ref, pair_ref, src_ref, text, passing,
                src_sem, w_sems, line_send, line_recv, row_send, row_recv, side_send, side_recv,
                twin_send, twin_recv, copy_sems):
    me = Place(dp, ctx)
    rows, planes, a, b, last = me.rows, me.planes, me.a, me.b, me.last
    share = ctx // dp
    width = own_ref.shape[2]
    features = share * width
    load_src = pltpu.make_async_copy(src_any, src_ref, src_sem)
    load_src.start()
    own_weights = pltpu.make_async_copy(weight_ref, pair_ref.at[0], w_sems.at[2])
    weights = remote(weight_ref, pair_ref.at[1], w_sems.at[0], w_sems.at[1], me.twin)
    me.greet()

    def slot(j, e, piece, core):
        at = (piece + core * share) % (2 * share) * width
        return text.at[e, j * 2 + me.core, :, pl.ds(pl.multiple_of(at, width), width)]

    def line(source, z, e, way, target):
        return remote(source, passing.at[z, e], line_send.at[z, e, way], line_recv.at[z, e], target)

    def to_row(source, z, e, j):
        row, i = z // share, z % share
        return remote(source, slot(j, e, i * 2 + b, me.core), row_send.at[z, e], row_recv.at[i, j, e], me.at_row(row))

    def to_side(source, i, j, e):
        return remote(source, slot(j, e, i * 2 + b, me.core), side_send.at[i, j, e], side_recv.at[i, j, e], me.side)

    def to_twin(source, piece, j, e):
        return remote(source, slot(j, e, piece, 1 - me.core), twin_send.at[piece, j, e],
                      twin_recv.at[piece, j, e], me.twin)

    def keep(source, i, e):
        return pltpu.make_async_copy(source, slot(me.row, e, i * 2 + b, me.core), copy_sems.at[i, e])

    def deliver(source, z, e):
        i = z % share

        @pl.when(z // share == me.row)
        def _():
            to_side(source, i, me.row, e).start()
            to_twin(source, i * 2 + b, me.row, e).start()
            keep(source, i, e).start()

        @pl.when(z // share != me.row)
        def _():
            to_row(source, z, e, me.row).start()

    def at_distance(s, body):
        for way in (0, 1) if s else (0,):
            z = a + s * (2 * way - 1)

            @pl.when((z >= 0) & (z <= last))
            def _():
                body(z, 1 - way)

    def arrive(z, way):
        target = me.up if way == 1 else me.down
        more = (a < last) if way == 1 else (a > 0)
        for e in range(2):
            source = passing.at[z, e]
            line(source, z, e, 0, me.up).wait_recv()

            @pl.when(more)
            def _():
                line(source, z, e, 1 - way, target).start()

            deliver(source, z, e)

    def from_rows(z, way):
        i = z % share

        @pl.when(z // share == me.row)
        def _():
            for j in range(rows):

                @pl.when(me.row != j)
                def _():
                    for e in range(2):
                        source = slot(j, e, i * 2 + b, me.core)
                        to_row(source, z, e, j).wait_recv()
                        to_side(source, i, j, e).start()
                        to_twin(source, i * 2 + b, j, e).start()

    def from_side(z, way):
        i = z % share

        @pl.when(z // share == me.row)
        def _():
            for j_at in range(rows):
                j = (me.row + j_at) % rows
                for e in range(2):
                    to_side(own_ref.at[e], i, j, e).wait_recv()
                    piece = i * 2 + 1 - b
                    to_twin(slot(j, e, piece, me.core), piece, j, e).start()

    for e in range(2):
        source = own_ref.at[e]

        @pl.when(a < last)
        def _():
            line(source, a, e, 0, me.up).start()

        @pl.when(a > 0)
        def _():
            line(source, a, e, 1, me.down).start()

        deliver(source, a, e)
    weights.start()
    own_weights.start()
    for s in range(1, planes + 2):
        if s < planes:
            at_distance(s, arrive)
        if s <= planes:
            at_distance(s - 1, from_rows)
        if s >= 2:
            at_distance(s - 2, from_side)

    load_src.wait()
    for i in range(share):
        for e in range(2):
            keep(own_ref.at[e], i, e).wait()
    for piece in range(2 * share):
        for j in range(rows):
            for e in range(2):
                to_twin(own_ref.at[e], piece, j, e).wait_recv()
    for e in range(2):
        for b_at in range(dp):
            rows_ref[e, b_at] = text[e, src_ref[b_at], :, pl.ds(0, features)]
        for j in range(rows):
            chosen_ref[e, j] = text[e, src_ref[j * 2 + me.core]]
    weights.wait()
    own_weights.wait()
    for e in range(2):
        for piece in range(2 * share):
            for j in range(rows):
                to_twin(own_ref.at[e], piece, j, e).wait_send()
        for i in range(share):
            for j in range(rows):
                to_side(own_ref.at[e], i, j, e).wait_send()
        for z in range(planes):

            @pl.when(z // share != me.row)
            def _():
                to_row(own_ref.at[e], z, e, me.row).wait_send()

            @pl.when((a < last) & (z <= a))
            def _():
                line(own_ref.at[e], z, e, 0, me.up).wait_send()

            @pl.when((a > 0) & (z >= a))
            def _():
                line(own_ref.at[e], z, e, 1, me.down).wait_send()


def gather_text(src, own, weight, dp, ctx):
    tokens, width = own.shape[1:]
    share = ctx // dp
    rows = dp // 2
    kind = own.dtype
    pieces = 2 * share
    planes = ctx // 2
    return pl.pallas_call(
        functools.partial(text_kernel, dp, ctx),
        in_specs=[HBM, HBM, HBM],
        out_specs=[VMEM, VMEM, VMEM],
        out_shape=[
            jax.ShapeDtypeStruct((2, rows, tokens, pieces * width), kind),
            jax.ShapeDtypeStruct((2, dp, tokens, share * width), kind),
            jax.ShapeDtypeStruct((2,) + weight.shape, weight.dtype),
        ],
        scratch_shapes=[
            pltpu.SMEM(src.shape, src.dtype),
            pltpu.VMEM((2, dp, tokens, pieces * width), kind),
            pltpu.VMEM((planes, 2, tokens, width), kind),
            DMA,
            DMA((3,)),
            DMA((planes, 2, 2)),
            DMA((planes, 2)),
            DMA((planes, 2)),
            DMA((share, rows, 2)),
            DMA((share, rows, 2)),
            DMA((share, rows, 2)),
            DMA((pieces, rows, 2)),
            DMA((pieces, rows, 2)),
            DMA((share, 2)),
        ],
        compiler_params=pltpu.CompilerParams(collective_id=1, has_side_effects=True, vmem_limit_bytes=16 << 20),
        name="gather_text",
    )(src, own, weight)


def sublayer_kernel(dp, ctx, cut, src_any, lengths_any, part_ref, q_any, g_any, out_ref, gq_ref, grads_ref,
                    src_ref, lengths_ref, q_ref, g_ref, sums, kv, gkv, crossed0, risen0, fallen0, going0,
                    risen1, fallen1, going1, crossed1,
                    in_sems, y_send, y_recv, ag_send, ag_recv, x0_send, x0_recv,
                    up0_send, up0_recv, down0_send, down0_recv,
                    up1_send, up1_recv, down1_send, down1_recv, x1_send, x1_recv,
                    dp_send, dp_recv, twin_send):
    me = Place(dp, ctx)
    nrows, a, b, last = me.rows, me.a, me.b, me.last
    planes = me.planes
    rounds = kv.shape[0]
    keys = kv.shape[2]
    tokens = keys // 2
    own = me.c
    load_q = pltpu.make_async_copy(q_any, q_ref, in_sems.at[0])
    load_g = pltpu.make_async_copy(g_any, g_ref, in_sems.at[1])
    load_src = pltpu.make_async_copy(src_any, src_ref, in_sems.at[2])
    load_lengths = pltpu.make_async_copy(lengths_any, lengths_ref, in_sems.at[3])
    load_src.start()
    load_lengths.start()
    load_q.start()
    load_g.start()
    me.greet()
    parts = (pl.ds(0, cut), pl.ds(cut, keys - cut))

    def columns(r):
        return pl.ds(pl.multiple_of(r * PAIR, PAIR), PAIR)

    def partial(r, row, sender):
        return remote(part_ref.at[:, row, :, columns(r)], sums.at[r, sender], y_send.at[r, row],
                      y_recv.at[r, sender], me.at_row(row))

    def ag(r, part, block, way, target):
        where = kv.at[r, block, parts[part], :]
        return remote(where, where, ag_send.at[r, part, block, way], ag_recv.at[r, part, block], target)

    def ag_wait(r, part, block):
        ag(r, part, block, 2, me.side).wait_recv()

    def send_up(r, part, block):
        @pl.when(a < last)
        def _():
            ag(r, part, block, 0, me.up).start()

    def send_down(r, part, block):
        @pl.when(a > 0)
        def _():
            ag(r, part, block, 1, me.down).start()

    def start_round(r):
        for j in range(nrows):

            @pl.when(me.row != j)
            def _():
                partial(r, j, j).wait_recv()

        for e in range(2):
            total = part_ref[e, me.row, :, columns(r)]
            for j_at in range(1, nrows):
                total = total + sums[r, (me.row + j_at) % nrows, e]
            kv[r, own, e * tokens:(e + 1) * tokens, :] = total.astype(kv.dtype)
        ag(r, 1, own, 2, me.side).start()
        send_up(r, 0, own)
        send_down(r, 0, own)
        ag(r, 0, own, 2, me.side).start()
        send_up(r, 1, own)
        send_down(r, 1, own)

    def relay_side(r):
        block = a * 2 + 1 - b
        ag_wait(r, 1, block)
        send_up(r, 1, block)
        send_down(r, 1, block)

    def relay(r, base, send, unit):
        side = b if unit < 2 else 1 - b
        part = 0 if unit == 0 else 1
        ag_wait(r, part, base + side)
        send(r, part, base + side)
        if part == 0:
            ag(r, 0, base + side, 2, me.side).start()

    scale = 1.0 / math.sqrt(HEAD)
    position = lax.broadcasted_iota(jnp.int32, (1, keys), 1)
    load_src.wait()
    load_lengths.wait()
    text_at = src_ref[me.d]
    bound = jnp.where(position < tokens, lengths_ref[0, text_at], lengths_ref[1, text_at] + tokens)
    bias = jnp.where(position < bound, 0.0, -1e30).astype(jnp.float32)

    def attend(r, block):
        at = pl.ds(pl.multiple_of((block * rounds + r) * HEAD, HEAD), HEAD)
        q = q_ref[:, at]
        g = g_ref[:, at]
        key = kv[r, block, :, :HEAD]
        value = kv[r, block, :, HEAD:]
        scores = dot(q, key, ((1,), (1,))) * scale + bias
        grad_probs = dot(g, value, ((1,), (1,)))
        top = jnp.max(scores, axis=-1, keepdims=True)
        weights = jnp.exp(scores - top)
        probs = weights * (1.0 / jnp.sum(weights, axis=-1, keepdims=True))
        probs_low = probs.astype(jnp.bfloat16)
        delta = jnp.sum(probs * grad_probs, axis=-1, keepdims=True)
        grad_scores = (probs * (grad_probs - delta) * scale).astype(jnp.bfloat16)
        out_ref[:, at] = dot(probs_low, value, ((1,), (0,))).astype(jnp.bfloat16)
        gq_ref[:, at] = dot(grad_scores, key, ((1,), (0,))).astype(jnp.bfloat16)
        gkv[r, block, :, :HEAD] = dot(grad_scores, q, ((0,), (0,))).astype(gkv.dtype)
        gkv[r, block, :, HEAD:] = dot(probs_low, g, ((0,), (0,))).astype(gkv.dtype)

    def cross0(r, z):
        return remote(gkv.at[r, z * 2 + 1 - b, parts[0], :], crossed0.at[r, z], x0_send.at[r, z],
                      x0_recv.at[r, z], me.side)

    def work(r, s):
        @pl.loop(0, 4)
        def _(t):
            way, foreign = t // 2, t % 2
            far = s - foreign
            z = a + far * (2 * way - 1)
            block = z * 2 + b + foreign * (1 - 2 * b)

            @pl.when((z >= 0) & (z <= last) & (far >= 0) & (far <= last) & ((far > 0) | (way == 0)))
            def _():
                @pl.when(foreign == 1)
                def _():
                    ag_wait(r, 0, block)

                attend(r, block)

                @pl.when(foreign == 1)
                def _():
                    cross0(r, z).start()

    def chain0(r, z, rising):
        if rising:
            return remote(going0.at[r, z], risen0.at[r, z], up0_send.at[r, z], up0_recv.at[r, z], me.up)
        return remote(going0.at[r, z], fallen0.at[r, z], down0_send.at[r, z], down0_recv.at[r, z], me.down)

    def chain1(r, z, side, rising, source):
        if rising:
            return remote(source, risen1.at[r, z, side], up1_send.at[r, z, side], up1_recv.at[r, z, side], me.up)
        return remote(source, fallen1.at[r, z, side], down1_send.at[r, z, side], down1_recv.at[r, z, side], me.down)

    def add(target, terms):
        @pl.loop(0, target.shape[0] // STEP)
        def _(i):
            at = pl.ds(pl.multiple_of(i * STEP, STEP), STEP)
            total = terms[0][at, :].astype(jnp.float32)
            for term in terms[1:]:
                total = total + term[at, :].astype(jnp.float32)
            target[at, :] = total.astype(target.dtype)

    def pass_on(r, z, rising, begins, unit):
        arrived0 = risen0 if rising else fallen0
        arrived1 = risen1 if rising else fallen1
        if unit < 2:
            side = b if unit == 0 else 1 - b
            source = gkv.at[r, z * 2 + side, parts[1], :]
            if not begins:
                target = going1.at[r, z, side]
                chain1(r, z, side, rising, target).wait_recv()
                add(target, [source, arrived1.at[r, z, side]])
                source = target
            chain1(r, z, side, rising, source).start()
        else:
            cross0(r, z).wait_recv()
            terms = [gkv.at[r, z * 2 + b, parts[0], :], crossed0.at[r, z]]
            if not begins:
                chain0(r, z, rising).wait_recv()
                terms.append(arrived0.at[r, z])
            add(going0.at[r, z], terms)
            chain0(r, z, rising).start()

    def move(i, s, unit):
        @pl.when((i < rounds) & (a >= s))
        def _():
            relay(i, (a - s) * 2, send_up, unit)

        @pl.when((i > 0) & (a == 0))
        def _():
            pass_on(i - 1, last + 1 - s, True, True, unit)

        @pl.when((i > 0) & (a > 0) & (a < s))
        def _():
            pass_on(i - 1, last + a + 1 - s, True, False, unit)

        @pl.when((i < rounds) & (a + s <= last))
        def _():
            relay(i, (a + s) * 2, send_down, unit)

        @pl.when((i > 0) & (a == last))
        def _():
            pass_on(i - 1, s - 1, False, True, unit)

        @pl.when((i > 0) & (a < last) & (last - a < s))
        def _():
            pass_on(i - 1, s - last + a - 1, False, False, unit)

    def own_terms(r, low, high, side=None):
        terms = []
        if side is None:
            terms += [risen0.at[r, a]] * low + [fallen0.at[r, a]] * high
        else:
            terms += [risen1.at[r, a, side]] * low + [fallen1.at[r, a, side]] * high
        return terms

    def cross1(r):
        return remote(going1.at[r, a, 1 - b], crossed1.at[r], x1_send.at[r], x1_recv.at[r], me.side)

    def by_place(body):
        @pl.when(a == 0)
        def _():
            body(0, 1)

        @pl.when(a == last)
        def _():
            body(1, 0)

        @pl.when((a > 0) & (a < last))
        def _():
            body(1, 1)

    def finish(r):
        def body(low, high):
            for rising in (True,) * low + (False,) * high:
                for side in range(2):
                    chain1(r, a, side, rising, going1.at[r, a, side]).wait_recv()
            add(going1.at[r, a, 1 - b],
                [gkv.at[r, a * 2 + 1 - b, parts[1], :]] + own_terms(r, low, high, 1 - b))
            cross1(r).start()
            for rising in (True,) * low + (False,) * high:
                chain0(r, a, rising).wait_recv()
            cross0(r, a).wait_recv()
            add(grads_ref.at[me.d, parts[0], columns(r)],
                [gkv.at[r, own, parts[0], :], crossed0.at[r, a]] + own_terms(r, low, high))

        by_place(body)

    def share_grads(r, d, way, target):
        where = grads_ref.at[d, :, columns(r)]
        return remote(where, where, dp_send.at[r, way], dp_recv.at[r, d], target)

    def hand_over(r, d):
        where = grads_ref.at[d, :, columns(r)]
        return remote(where, where, twin_send.at[r, d // 2], dp_recv.at[r, d], me.twin)

    def close(r):
        cross1(r).wait_recv()

        def body(low, high):
            add(grads_ref.at[me.d, parts[1], columns(r)],
                [gkv.at[r, own, parts[1], :], crossed1.at[r]] + own_terms(r, low, high, b))

        by_place(body)
        for j in range(nrows):

            @pl.when(me.row != j)
            def _():
                share_grads(r, me.d, j, me.at_row(j)).start()

        hand_over(r, me.d).start()

    def spread(r):
        for j in range(nrows):

            @pl.when(me.row != j)
            def _():
                d = j * 2 + me.core
                share_grads(r, d, j, me.at_row(j)).wait_recv()
                hand_over(r, d).start()

    @pl.loop(0, rounds)
    def _(r):
        for j in range(nrows):

            @pl.when(me.row != j)
            def _():
                partial(r, j, me.row).start()

    start_round(0)
    load_q.wait()
    load_g.wait()

    @pl.loop(0, rounds + 1)
    def _(i):
        for s in range(planes):

            if s == 0:

                @pl.when(i < rounds)
                def _():
                    relay_side(i)

            else:
                for unit in range(3):
                    move(i, s, unit)

            if s == last:

                @pl.when(i + 1 < rounds)
                def _():
                    start_round(i + 1)

            if s == min(1, last):

                @pl.when(i > 1)
                def _():
                    finish(i - 2)

            if s == min(2, last):

                @pl.when(i > 1)
                def _():
                    close(i - 2)

            if s == last:

                @pl.when(i > 2)
                def _():
                    spread(i - 3)

            @pl.when(i < rounds)
            def _():
                work(i, s)

        @pl.when(i < rounds)
        def _():
            work(i, planes)

    finish(rounds - 1)
    close(rounds - 1)
    for r in range(max(rounds - 2, 0), rounds):
        spread(r)

    @pl.loop(0, rounds)
    def _(r):
        for j in range(nrows):
            hand_over(r, j * 2 + 1 - me.core).wait_recv()
            hand_over(r, j * 2 + me.core).wait_send()

            @pl.when(me.row != j)
            def _():
                partial(r, j, me.row).wait_send()
                share_grads(r, me.d, j, me.at_row(j)).wait_send()

        ag(r, 1, own, 2, me.side).wait_send()
        cross1(r).wait_send()
        for z in range(planes):
            cross0(r, z).wait_send()
            ag(r, 0, z * 2 + b, 2, me.side).wait_send()

            @pl.when((a < last) & (z <= a))
            def _():
                ag(r, 0, z * 2 + b, 0, me.up).wait_send()
                for side in range(2):
                    ag(r, 1, z * 2 + side, 0, me.up).wait_send()

            @pl.when((a > 0) & (z >= a))
            def _():
                ag(r, 0, z * 2 + b, 1, me.down).wait_send()
                for side in range(2):
                    ag(r, 1, z * 2 + side, 1, me.down).wait_send()

            for rising in (True, False):

                @pl.when((z > a) if rising else (z < a))
                def _():
                    chain0(r, z, rising).wait_send()
                    for side in range(2):
                        chain1(r, z, side, rising, going1.at[r, z, side]).wait_send()


def sublayer(src, lengths, part, queries, grad_out, dp, ctx):
    _, rows, tokens, columns = part.shape
    rounds = columns // PAIR
    keys = 2 * tokens
    planes = ctx // 2
    cut = keys * 5 // 8 // STEP * STEP
    low = jnp.bfloat16
    first = pltpu.VMEM((rounds, planes, cut, PAIR), low)
    second = pltpu.VMEM((rounds, planes, 2, keys - cut, PAIR), low)
    whole = pltpu.VMEM((rounds, ctx, keys, PAIR), low)
    return pl.pallas_call(
        functools.partial(sublayer_kernel, dp, ctx, cut),
        in_specs=[HBM, HBM, VMEM, HBM, HBM],
        out_specs=[VMEM, VMEM, VMEM],
        out_shape=[
            jax.ShapeDtypeStruct(queries.shape, low),
            jax.ShapeDtypeStruct(queries.shape, low),
            jax.ShapeDtypeStruct((dp, keys, columns), low),
        ],
        scratch_shapes=[
            pltpu.SMEM(src.shape, src.dtype),
            pltpu.SMEM(lengths.shape, lengths.dtype),
            pltpu.VMEM(queries.shape, low),
            pltpu.VMEM(queries.shape, low),
            pltpu.VMEM((rounds, rows, 2, tokens, PAIR), jnp.float32),
            whole,
            whole,
            first,
            first,
            first,
            first,
            second,
            second,
            second,
            pltpu.VMEM((rounds, keys - cut, PAIR), low),
            DMA((4,)),
            DMA((rounds, rows)),
            DMA((rounds, rows)),
            DMA((rounds, 2, ctx, 3)),
            DMA((rounds, 2, ctx)),
        ]
        + [DMA((rounds, planes))] * 6
        + [DMA((rounds, planes, 2))] * 4
        + [
            DMA((rounds,)),
            DMA((rounds,)),
            DMA((rounds, rows)),
            DMA((rounds, dp)),
            DMA((rounds, rows)),
        ],
        compiler_params=pltpu.CompilerParams(collective_id=2, has_side_effects=True, vmem_limit_bytes=36 << 20),
        name="sublayer",
    )(src, lengths, part, queries, grad_out)


def weight_kernel(rows_ref, grads_ref, att_ref, gq_ref, out_ref, att_out, gq_out, buffer, sems):
    keep_att = pltpu.make_async_copy(att_ref, att_out, sems.at[0])
    keep_gq = pltpu.make_async_copy(gq_ref, gq_out, sems.at[1])
    keep_att.start()
    keep_gq.start()
    dp, keys, columns = grads_ref.shape
    tokens = keys // 2
    features = rows_ref.shape[3]
    lanes = columns // HEAD
    stride = 2 * lanes
    size = HEAD

    def ship(i):
        at = pl.ds(i * size * stride, size * stride)
        return pltpu.make_async_copy(buffer.at[at, :], out_ref.at[at, :], sems.at[2 + i])

    for i in range(features // size):
        for e in range(2):
            left = rows_ref[e, :, :, i * size:(i + 1) * size].reshape(dp * tokens, size)
            for j in range(columns // PAIR):
                right = grads_ref[:, e * tokens:(e + 1) * tokens, j * PAIR:(j + 1) * PAIR].reshape(dp * tokens, PAIR)
                block = dot(left, right, ((0,), (0,)))
                for half in range(2):
                    buffer[pl.ds(i * size * stride + (2 * j + half) * 2 + e, size, stride), :] = (
                        block[:, half * HEAD:(half + 1) * HEAD]
                    )
        ship(i).start()
    for i in range(features // size):
        ship(i).wait()
    keep_att.wait()
    keep_gq.wait()


def finish_weight(rows, grads, attended, grad_queries):
    dp, keys, columns = grads.shape
    features = rows.shape[3]
    lanes = columns // HEAD
    flat = (features * lanes * 2, HEAD)
    weight, attended, grad_queries = pl.pallas_call(
        weight_kernel,
        in_specs=[VMEM, VMEM, VMEM, VMEM],
        out_specs=[ANY, ANY, ANY],
        out_shape=[
            jax.ShapeDtypeStruct(flat, jnp.float32),
            jax.ShapeDtypeStruct(attended.shape, attended.dtype),
            jax.ShapeDtypeStruct(attended.shape, attended.dtype),
        ],
        scratch_shapes=[pltpu.VMEM(flat, jnp.float32), DMA((2 + features // HEAD,))],
        compiler_params=pltpu.CompilerParams(vmem_limit_bytes=24 << 20),
        name="finish_weight",
    )(rows, grads, attended, grad_queries)
    weight = weight.reshape(features, lanes, 2, HEAD).transpose(0, 2, 1, 3).reshape(features, 2, columns)
    return attended, grad_queries, weight


def per_device(dp, ctx, text, src, lengths, kv_weight, queries, grad_out):
    chosen, rows, pair = gather_text(src, text[0], kv_weight, dp, ctx)
    dims = "ejtf,fec->ejtc"
    pair = pair.reshape((-1,) + kv_weight.shape[1:])
    part = jnp.einsum(dims, chosen, pair, preferred_element_type=jnp.float32)
    attended, grad_queries, grads = sublayer(src, lengths.T, part, queries[0], grad_out[0], dp, ctx)
    attended, grad_queries, weight = finish_weight(rows, grads, attended, grad_queries)
    return (attended[None], grad_queries[None], weight)


def solution(mesh):
    placed = (
        P("dp", None, None, "ctx"),
        P(),
        P(),
        P("dp", None, "ctx"),
        P("dp", "ctx", None),
        P("dp", "ctx", None),
    )
    return jax.shard_map(
        functools.partial(per_device, mesh.shape["dp"], mesh.shape["ctx"]),
        mesh=mesh,
        in_specs=placed,
        out_specs=(P("dp", "ctx", None), P("dp", "ctx", None), P("dp", None, "ctx")),
        check_vma=False,
    )
```

```python
import functools
import math

import jax
import jax.numpy as jnp
from jax import lax
from jax.experimental import pallas as pl
from jax.experimental.pallas import tpu as pltpu
from jax.sharding import PartitionSpec as P

HEAD = 128
PAIR = 2 * HEAD
STEP = 32
MESH = pl.DeviceIdType.MESH
VMEM = pl.BlockSpec(memory_space=pltpu.VMEM)
SMEM = pl.BlockSpec(memory_space=pltpu.SMEM)
ANY = pl.BlockSpec(memory_space=pl.ANY)
HBM = pl.BlockSpec(memory_space=pltpu.HBM)
DMA = pltpu.SemaphoreType.DMA


def dot(a, b, dims):
    return lax.dot_general(a, b, (dims, ((), ())), preferred_element_type=jnp.float32)


def remote(src, dst, send_sem, recv_sem, target):
    return pltpu.make_async_remote_copy(
        src_ref=src, dst_ref=dst, send_sem=send_sem, recv_sem=recv_sem, device_id=target, device_id_type=MESH
    )


class Place:
    def __init__(self, dp, ctx):
        self.rows, self.planes = dp // 2, ctx // 2
        self.last = self.planes - 1
        self.d, self.c = lax.axis_index("dp"), lax.axis_index("ctx")
        self.row, self.core = self.d // 2, self.d % 2
        self.a, self.b = self.c // 2, self.c % 2
        self.up = {"ctx": self.c + 2}
        self.down = {"ctx": self.c - 2}
        self.side = {"ctx": self.a * 2 + 1 - self.b}
        self.twin = {"dp": self.row * 2 + 1 - self.core}

    def at_row(self, row):
        return {"dp": row * 2 + self.core}

    def greet(self):
        barrier = pltpu.get_barrier_semaphore()

        def hello(target):
            pl.semaphore_signal(barrier, inc=1, device_id=target, device_id_type=MESH)

        hello(self.side)
        hello(self.twin)
        for j in range(self.rows):

            @pl.when(self.row != j)
            def _():
                hello(self.at_row(j))

        @pl.when(self.a < self.last)
        def _():
            hello(self.up)

        @pl.when(self.a > 0)
        def _():
            hello(self.down)

        fixed = 1 + self.rows
        if self.last == 0:
            pl.semaphore_wait(barrier, fixed)
        else:

            @pl.when((self.a > 0) & (self.a < self.last))
            def _():
                pl.semaphore_wait(barrier, fixed + 2)

            @pl.when((self.a == 0) | (self.a == self.last))
            def _():
                pl.semaphore_wait(barrier, fixed + 1)


def text_kernel(dp, ctx, src_any, own_ref, weight_ref, chosen_ref, rows_ref, pair_ref, src_ref, text, passing,
                src_sem, w_sems, line_send, line_recv, row_send, row_recv, side_send, side_recv,
                twin_send, twin_recv, copy_sems):
    me = Place(dp, ctx)
    rows, planes, a, b, last = me.rows, me.planes, me.a, me.b, me.last
    share = ctx // dp
    width = own_ref.shape[2]
    features = share * width
    load_src = pltpu.make_async_copy(src_any, src_ref, src_sem)
    load_src.start()
    own_weights = pltpu.make_async_copy(weight_ref, pair_ref.at[0], w_sems.at[2])
    weights = remote(weight_ref, pair_ref.at[1], w_sems.at[0], w_sems.at[1], me.twin)
    me.greet()

    def slot(j, e, piece, core):
        at = (piece + core * share) % (2 * share) * width
        return text.at[e, j * 2 + me.core, :, pl.ds(pl.multiple_of(at, width), width)]

    def line(source, z, e, way, target):
        return remote(source, passing.at[z, e], line_send.at[z, e, way], line_recv.at[z, e], target)

    def to_row(source, z, e, j):
        row, i = z // share, z % share
        return remote(source, slot(j, e, i * 2 + b, me.core), row_send.at[z, e], row_recv.at[i, j, e], me.at_row(row))

    def to_side(source, i, j, e):
        return remote(source, slot(j, e, i * 2 + b, me.core), side_send.at[i, j, e], side_recv.at[i, j, e], me.side)

    def to_twin(source, piece, j, e):
        return remote(source, slot(j, e, piece, 1 - me.core), twin_send.at[piece, j, e],
                      twin_recv.at[piece, j, e], me.twin)

    def keep(source, i, e):
        return pltpu.make_async_copy(source, slot(me.row, e, i * 2 + b, me.core), copy_sems.at[i, e])

    def deliver(source, z, e):
        i = z % share

        @pl.when(z // share == me.row)
        def _():
            to_side(source, i, me.row, e).start()
            to_twin(source, i * 2 + b, me.row, e).start()
            keep(source, i, e).start()

        @pl.when(z // share != me.row)
        def _():
            to_row(source, z, e, me.row).start()

    def at_distance(s, body):
        for way in (0, 1) if s else (0,):
            z = a + s * (2 * way - 1)

            @pl.when((z >= 0) & (z <= last))
            def _():
                body(z, 1 - way)

    def arrive(z, way):
        target = me.up if way == 1 else me.down
        more = (a < last) if way == 1 else (a > 0)
        for e in range(2):
            source = passing.at[z, e]
            line(source, z, e, 0, me.up).wait_recv()

            @pl.when(more)
            def _():
                line(source, z, e, 1 - way, target).start()

            deliver(source, z, e)

    def from_rows(z, way):
        i = z % share

        @pl.when(z // share == me.row)
        def _():
            for j in range(rows):

                @pl.when(me.row != j)
                def _():
                    for e in range(2):
                        source = slot(j, e, i * 2 + b, me.core)
                        to_row(source, z, e, j).wait_recv()
                        to_side(source, i, j, e).start()
                        to_twin(source, i * 2 + b, j, e).start()

    def from_side(z, way):
        i = z % share

        @pl.when(z // share == me.row)
        def _():
            for j_at in range(rows):
                j = (me.row + j_at) % rows
                for e in range(2):
                    to_side(own_ref.at[e], i, j, e).wait_recv()
                    piece = i * 2 + 1 - b
                    to_twin(slot(j, e, piece, me.core), piece, j, e).start()

    for e in range(2):
        source = own_ref.at[e]

        @pl.when(a < last)
        def _():
            line(source, a, e, 0, me.up).start()

        @pl.when(a > 0)
        def _():
            line(source, a, e, 1, me.down).start()

        deliver(source, a, e)
    weights.start()
    own_weights.start()
    for s in range(1, planes + 2):
        if s < planes:
            at_distance(s, arrive)
        if s <= planes:
            at_distance(s - 1, from_rows)
        if s >= 2:
            at_distance(s - 2, from_side)

    load_src.wait()
    for i in range(share):
        for e in range(2):
            keep(own_ref.at[e], i, e).wait()
    for piece in range(2 * share):
        for j in range(rows):
            for e in range(2):
                to_twin(own_ref.at[e], piece, j, e).wait_recv()
    for e in range(2):
        for b_at in range(dp):
            rows_ref[e, b_at] = text[e, src_ref[b_at], :, pl.ds(0, features)]
        for j in range(rows):
            chosen_ref[e, j] = text[e, src_ref[j * 2 + me.core]]
    weights.wait()
    own_weights.wait()
    for e in range(2):
        for piece in range(2 * share):
            for j in range(rows):
                to_twin(own_ref.at[e], piece, j, e).wait_send()
        for i in range(share):
            for j in range(rows):
                to_side(own_ref.at[e], i, j, e).wait_send()
        for z in range(planes):

            @pl.when(z // share != me.row)
            def _():
                to_row(own_ref.at[e], z, e, me.row).wait_send()

            @pl.when((a < last) & (z <= a))
            def _():
                line(own_ref.at[e], z, e, 0, me.up).wait_send()

            @pl.when((a > 0) & (z >= a))
            def _():
                line(own_ref.at[e], z, e, 1, me.down).wait_send()


def gather_text(src, own, weight, dp, ctx):
    tokens, width = own.shape[1:]
    share = ctx // dp
    rows = dp // 2
    kind = own.dtype
    pieces = 2 * share
    planes = ctx // 2
    return pl.pallas_call(
        functools.partial(text_kernel, dp, ctx),
        in_specs=[HBM, HBM, HBM],
        out_specs=[VMEM, VMEM, VMEM],
        out_shape=[
            jax.ShapeDtypeStruct((2, rows, tokens, pieces * width), kind),
            jax.ShapeDtypeStruct((2, dp, tokens, share * width), kind),
            jax.ShapeDtypeStruct((2,) + weight.shape, weight.dtype),
        ],
        scratch_shapes=[
            pltpu.SMEM(src.shape, src.dtype),
            pltpu.VMEM((2, dp, tokens, pieces * width), kind),
            pltpu.VMEM((planes, 2, tokens, width), kind),
            DMA,
            DMA((3,)),
            DMA((planes, 2, 2)),
            DMA((planes, 2)),
            DMA((planes, 2)),
            DMA((share, rows, 2)),
            DMA((share, rows, 2)),
            DMA((share, rows, 2)),
            DMA((pieces, rows, 2)),
            DMA((pieces, rows, 2)),
            DMA((share, 2)),
        ],
        compiler_params=pltpu.CompilerParams(collective_id=1, has_side_effects=True, vmem_limit_bytes=16 << 20),
        name="gather_text",
    )(src, own, weight)


def sublayer_kernel(dp, ctx, cut, src_any, lengths_any, part_ref, q_any, g_any, out_ref, gq_ref, grads_ref,
                    src_ref, lengths_ref, q_ref, g_ref, sums, kv, gkv, crossed0, risen0, fallen0, going0,
                    risen1, fallen1, going1, crossed1,
                    in_sems, y_send, y_recv, ag_send, ag_recv, x0_send, x0_recv,
                    up0_send, up0_recv, down0_send, down0_recv,
                    up1_send, up1_recv, down1_send, down1_recv, x1_send, x1_recv,
                    dp_send, dp_recv, twin_send):
    me = Place(dp, ctx)
    nrows, a, b, last = me.rows, me.a, me.b, me.last
    planes = me.planes
    rounds = kv.shape[0]
    keys = kv.shape[2]
    tokens = keys // 2
    own = me.c
    load_q = pltpu.make_async_copy(q_any, q_ref, in_sems.at[0])
    load_g = pltpu.make_async_copy(g_any, g_ref, in_sems.at[1])
    load_src = pltpu.make_async_copy(src_any, src_ref, in_sems.at[2])
    load_lengths = pltpu.make_async_copy(lengths_any, lengths_ref, in_sems.at[3])
    load_src.start()
    load_lengths.start()
    load_q.start()
    load_g.start()
    me.greet()
    parts = (pl.ds(0, cut), pl.ds(cut, keys - cut))
    pieces = ((1, cut - tokens, tokens), (0, 0, tokens), (1, 0, cut - tokens))

    def columns(r):
        return pl.ds(pl.multiple_of(r * PAIR, PAIR), PAIR)

    def partial(r, row, sender, piece):
        e, low, high = pieces[piece]
        return remote(part_ref.at[e, row, low:high, columns(r)], sums.at[r, sender, e, low:high, :],
                      y_send.at[r, row, piece], y_recv.at[r, sender, piece], me.at_row(row))

    def total(r, piece):
        e, low, high = pieces[piece]
        for j in range(nrows):

            @pl.when(me.row != j)
            def _():
                partial(r, j, j, piece).wait_recv()

        value = part_ref[e, me.row, low:high, columns(r)]
        for j_at in range(1, nrows):
            value = value + sums[r, (me.row + j_at) % nrows, e, low:high, :]
        kv[r, own, e * tokens + low:e * tokens + high, :] = value.astype(kv.dtype)

    def ag(r, part, block, way, target):
        where = kv.at[r, block, parts[part], :]
        return remote(where, where, ag_send.at[r, part, block, way], ag_recv.at[r, part, block], target)

    def ag_wait(r, part, block):
        ag(r, part, block, 2, me.side).wait_recv()

    def send_up(r, part, block):
        @pl.when(a < last)
        def _():
            ag(r, part, block, 0, me.up).start()

    def send_down(r, part, block):
        @pl.when(a > 0)
        def _():
            ag(r, part, block, 1, me.down).start()

    def start_round(r, early=False):
        total(r, 0)
        ag(r, 1, own, 2, me.side).start()
        if early:
            send_up(r, 1, own)
            send_down(r, 1, own)
        total(r, 1)
        total(r, 2)
        send_up(r, 0, own)
        send_down(r, 0, own)
        ag(r, 0, own, 2, me.side).start()
        if not early:
            send_up(r, 1, own)
            send_down(r, 1, own)

    def relay_side(r):
        block = a * 2 + 1 - b
        ag_wait(r, 1, block)
        send_up(r, 1, block)
        send_down(r, 1, block)

    def relay(r, base, send, unit):
        side = b if unit < 2 else 1 - b
        part = 0 if unit == 0 else 1
        ag_wait(r, part, base + side)
        send(r, part, base + side)
        if part == 0:
            ag(r, 0, base + side, 2, me.side).start()

    scale = 1.0 / math.sqrt(HEAD)
    position = lax.broadcasted_iota(jnp.int32, (1, keys), 1)
    load_src.wait()
    load_lengths.wait()
    text_at = src_ref[me.d]
    bound = jnp.where(position < tokens, lengths_ref[0, text_at], lengths_ref[1, text_at] + tokens)
    bias = jnp.where(position < bound, 0.0, -1e30).astype(jnp.float32)

    def attend(r, block):
        at = pl.ds(pl.multiple_of((block * rounds + r) * HEAD, HEAD), HEAD)
        q = q_ref[:, at]
        g = g_ref[:, at]
        key = kv[r, block, :, :HEAD]
        value = kv[r, block, :, HEAD:]
        scores = dot(q, key, ((1,), (1,))) * scale + bias
        grad_probs = dot(g, value, ((1,), (1,)))
        top = jnp.max(scores, axis=-1, keepdims=True)
        weights = jnp.exp(scores - top)
        probs = weights * (1.0 / jnp.sum(weights, axis=-1, keepdims=True))
        probs_low = probs.astype(jnp.bfloat16)
        delta = jnp.sum(probs * grad_probs, axis=-1, keepdims=True)
        grad_scores = (probs * (grad_probs - delta) * scale).astype(jnp.bfloat16)
        out_ref[:, at] = dot(probs_low, value, ((1,), (0,))).astype(jnp.bfloat16)
        gq_ref[:, at] = dot(grad_scores, key, ((1,), (0,))).astype(jnp.bfloat16)
        gkv[r, block, :, :HEAD] = dot(grad_scores, q, ((0,), (0,))).astype(gkv.dtype)
        gkv[r, block, :, HEAD:] = dot(probs_low, g, ((0,), (0,))).astype(gkv.dtype)

    def cross0(r, z):
        return remote(gkv.at[r, z * 2 + 1 - b, parts[0], :], crossed0.at[r, z], x0_send.at[r, z],
                      x0_recv.at[r, z], me.side)

    def work(r, s):
        @pl.loop(0, 4)
        def _(t):
            way, foreign = t // 2, t % 2
            far = s - foreign
            z = a + far * (2 * way - 1)
            block = z * 2 + b + foreign * (1 - 2 * b)

            @pl.when((z >= 0) & (z <= last) & (far >= 0) & (far <= last) & ((far > 0) | (way == 0)))
            def _():
                @pl.when(foreign == 1)
                def _():
                    ag_wait(r, 0, block)

                attend(r, block)

                @pl.when(foreign == 1)
                def _():
                    cross0(r, z).start()

    def chain0(r, z, rising):
        if rising:
            return remote(going0.at[r, z], risen0.at[r, z], up0_send.at[r, z], up0_recv.at[r, z], me.up)
        return remote(going0.at[r, z], fallen0.at[r, z], down0_send.at[r, z], down0_recv.at[r, z], me.down)

    def chain1(r, z, side, rising, source):
        if rising:
            return remote(source, risen1.at[r, z, side], up1_send.at[r, z, side], up1_recv.at[r, z, side], me.up)
        return remote(source, fallen1.at[r, z, side], down1_send.at[r, z, side], down1_recv.at[r, z, side], me.down)

    def add(target, terms):
        @pl.loop(0, target.shape[0] // STEP)
        def _(i):
            at = pl.ds(pl.multiple_of(i * STEP, STEP), STEP)
            total = terms[0][at, :].astype(jnp.float32)
            for term in terms[1:]:
                total = total + term[at, :].astype(jnp.float32)
            target[at, :] = total.astype(target.dtype)

    def pass_on(r, z, rising, begins, unit):
        arrived0 = risen0 if rising else fallen0
        arrived1 = risen1 if rising else fallen1
        if unit < 2:
            side = b if unit == 0 else 1 - b
            source = gkv.at[r, z * 2 + side, parts[1], :]
            if not begins:
                target = going1.at[r, z, side]
                chain1(r, z, side, rising, target).wait_recv()
                add(target, [source, arrived1.at[r, z, side]])
                source = target
            chain1(r, z, side, rising, source).start()
        else:
            cross0(r, z).wait_recv()
            terms = [gkv.at[r, z * 2 + b, parts[0], :], crossed0.at[r, z]]
            if not begins:
                chain0(r, z, rising).wait_recv()
                terms.append(arrived0.at[r, z])
            add(going0.at[r, z], terms)
            chain0(r, z, rising).start()

    def move(i, s, unit):
        @pl.when((i < rounds) & (a >= s))
        def _():
            relay(i, (a - s) * 2, send_up, unit)

        @pl.when((i > 0) & (a == 0))
        def _():
            pass_on(i - 1, last + 1 - s, True, True, unit)

        @pl.when((i > 0) & (a > 0) & (a < s))
        def _():
            pass_on(i - 1, last + a + 1 - s, True, False, unit)

        @pl.when((i < rounds) & (a + s <= last))
        def _():
            relay(i, (a + s) * 2, send_down, unit)

        @pl.when((i > 0) & (a == last))
        def _():
            pass_on(i - 1, s - 1, False, True, unit)

        @pl.when((i > 0) & (a < last) & (last - a < s))
        def _():
            pass_on(i - 1, s - last + a - 1, False, False, unit)

    def own_terms(r, low, high, side=None):
        terms = []
        if side is None:
            terms += [risen0.at[r, a]] * low + [fallen0.at[r, a]] * high
        else:
            terms += [risen1.at[r, a, side]] * low + [fallen1.at[r, a, side]] * high
        return terms

    def cross1(r):
        return remote(going1.at[r, a, 1 - b], crossed1.at[r], x1_send.at[r], x1_recv.at[r], me.side)

    def by_place(body):
        @pl.when(a == 0)
        def _():
            body(0, 1)

        @pl.when(a == last)
        def _():
            body(1, 0)

        @pl.when((a > 0) & (a < last))
        def _():
            body(1, 1)

    def finish(r):
        def body(low, high):
            for rising in (True,) * low + (False,) * high:
                for side in range(2):
                    chain1(r, a, side, rising, going1.at[r, a, side]).wait_recv()
            add(going1.at[r, a, 1 - b],
                [gkv.at[r, a * 2 + 1 - b, parts[1], :]] + own_terms(r, low, high, 1 - b))
            cross1(r).start()
            for rising in (True,) * low + (False,) * high:
                chain0(r, a, rising).wait_recv()
            cross0(r, a).wait_recv()
            add(grads_ref.at[me.d, parts[0], columns(r)],
                [gkv.at[r, own, parts[0], :], crossed0.at[r, a]] + own_terms(r, low, high))

        by_place(body)
        publish(r, 0)

    def share_grads(r, part, d, way, target):
        where = grads_ref.at[d, parts[part], columns(r)]
        return remote(where, where, dp_send.at[r, part, way], dp_recv.at[r, part, d], target)

    def hand_over(r, part, d):
        where = grads_ref.at[d, parts[part], columns(r)]
        return remote(where, where, twin_send.at[r, part, d // 2], dp_recv.at[r, part, d], me.twin)

    def publish(r, part):
        for j in range(nrows):

            @pl.when(me.row != j)
            def _():
                share_grads(r, part, me.d, j, me.at_row(j)).start()

        hand_over(r, part, me.d).start()

    def close(r):
        cross1(r).wait_recv()

        def body(low, high):
            add(grads_ref.at[me.d, parts[1], columns(r)],
                [gkv.at[r, own, parts[1], :], crossed1.at[r]] + own_terms(r, low, high, b))

        by_place(body)
        publish(r, 1)

    def spread(r):
        for part in range(2):
            for j in range(nrows):

                @pl.when(me.row != j)
                def _():
                    d = j * 2 + me.core
                    share_grads(r, part, d, j, me.at_row(j)).wait_recv()
                    hand_over(r, part, d).start()

    @pl.loop(0, rounds)
    def _(r):
        for j in range(nrows):

            @pl.when(me.row != j)
            def _():
                for piece in range(3):
                    partial(r, j, me.row, piece).start()

    start_round(0, True)
    load_q.wait()
    load_g.wait()

    @pl.loop(0, rounds + 1)
    def _(i):
        for s in range(planes):

            if s == 0:

                @pl.when(i < rounds)
                def _():
                    relay_side(i)

            else:
                for unit in range(3):
                    move(i, s, unit)

            if s == last:

                @pl.when(i + 1 < rounds)
                def _():
                    start_round(i + 1)

            if s == min(1, last):

                @pl.when(i > 1)
                def _():
                    finish(i - 2)

            if s == min(2, last):

                @pl.when(i > 1)
                def _():
                    close(i - 2)

            if s == last:

                @pl.when(i > 2)
                def _():
                    spread(i - 3)

            @pl.when(i < rounds)
            def _():
                work(i, s)

        @pl.when(i < rounds)
        def _():
            work(i, planes)

    finish(rounds - 1)
    close(rounds - 1)
    for r in range(max(rounds - 2, 0), rounds):
        spread(r)

    @pl.loop(0, rounds)
    def _(r):
        for j in range(nrows):
            for part in range(2):
                hand_over(r, part, j * 2 + 1 - me.core).wait_recv()
                hand_over(r, part, j * 2 + me.core).wait_send()

            @pl.when(me.row != j)
            def _():
                for piece in range(3):
                    partial(r, j, me.row, piece).wait_send()
                for part in range(2):
                    share_grads(r, part, me.d, j, me.at_row(j)).wait_send()

        ag(r, 1, own, 2, me.side).wait_send()
        cross1(r).wait_send()
        for z in range(planes):
            cross0(r, z).wait_send()
            ag(r, 0, z * 2 + b, 2, me.side).wait_send()

            @pl.when((a < last) & (z <= a))
            def _():
                ag(r, 0, z * 2 + b, 0, me.up).wait_send()
                for side in range(2):
                    ag(r, 1, z * 2 + side, 0, me.up).wait_send()

            @pl.when((a > 0) & (z >= a))
            def _():
                ag(r, 0, z * 2 + b, 1, me.down).wait_send()
                for side in range(2):
                    ag(r, 1, z * 2 + side, 1, me.down).wait_send()

            for rising in (True, False):

                @pl.when((z > a) if rising else (z < a))
                def _():
                    chain0(r, z, rising).wait_send()
                    for side in range(2):
                        chain1(r, z, side, rising, going1.at[r, z, side]).wait_send()


def sublayer(src, lengths, part, queries, grad_out, dp, ctx):
    _, rows, tokens, columns = part.shape
    rounds = columns // PAIR
    keys = 2 * tokens
    planes = ctx // 2
    cut = keys * 5 // 8 // STEP * STEP
    low = jnp.bfloat16
    first = pltpu.VMEM((rounds, planes, cut, PAIR), low)
    second = pltpu.VMEM((rounds, planes, 2, keys - cut, PAIR), low)
    whole = pltpu.VMEM((rounds, ctx, keys, PAIR), low)
    return pl.pallas_call(
        functools.partial(sublayer_kernel, dp, ctx, cut),
        in_specs=[HBM, HBM, VMEM, HBM, HBM],
        out_specs=[VMEM, VMEM, VMEM],
        out_shape=[
            jax.ShapeDtypeStruct(queries.shape, low),
            jax.ShapeDtypeStruct(queries.shape, low),
            jax.ShapeDtypeStruct((dp, keys, columns), low),
        ],
        scratch_shapes=[
            pltpu.SMEM(src.shape, src.dtype),
            pltpu.SMEM(lengths.shape, lengths.dtype),
            pltpu.VMEM(queries.shape, low),
            pltpu.VMEM(queries.shape, low),
            pltpu.VMEM((rounds, rows, 2, tokens, PAIR), jnp.float32),
            whole,
            whole,
            first,
            first,
            first,
            first,
            second,
            second,
            second,
            pltpu.VMEM((rounds, keys - cut, PAIR), low),
            DMA((4,)),
            DMA((rounds, rows, 3)),
            DMA((rounds, rows, 3)),
            DMA((rounds, 2, ctx, 3)),
            DMA((rounds, 2, ctx)),
        ]
        + [DMA((rounds, planes))] * 6
        + [DMA((rounds, planes, 2))] * 4
        + [
            DMA((rounds,)),
            DMA((rounds,)),
            DMA((rounds, 2, rows)),
            DMA((rounds, 2, dp)),
            DMA((rounds, 2, rows)),
        ],
        compiler_params=pltpu.CompilerParams(collective_id=2, has_side_effects=True, vmem_limit_bytes=44 << 20),
        name="sublayer",
    )(src, lengths, part, queries, grad_out)


def weight_kernel(rows_ref, grads_ref, att_ref, gq_ref, out_ref, att_out, gq_out, buffer, sems):
    keep_att = pltpu.make_async_copy(att_ref, att_out, sems.at[0])
    keep_gq = pltpu.make_async_copy(gq_ref, gq_out, sems.at[1])
    keep_att.start()
    keep_gq.start()
    dp, keys, columns = grads_ref.shape
    tokens = keys // 2
    features = rows_ref.shape[3]
    lanes = columns // HEAD
    stride = 2 * lanes
    size = HEAD

    def ship(i):
        at = pl.ds(i * size * stride, size * stride)
        return pltpu.make_async_copy(buffer.at[at, :], out_ref.at[at, :], sems.at[2 + i])

    for i in range(features // size):
        for e in range(2):
            left = rows_ref[e, :, :, i * size:(i + 1) * size].reshape(dp * tokens, size)
            for j in range(columns // PAIR):
                right = grads_ref[:, e * tokens:(e + 1) * tokens, j * PAIR:(j + 1) * PAIR].reshape(dp * tokens, PAIR)
                block = dot(left, right, ((0,), (0,)))
                for half in range(2):
                    buffer[pl.ds(i * size * stride + (2 * j + half) * 2 + e, size, stride), :] = (
                        block[:, half * HEAD:(half + 1) * HEAD]
                    )
        ship(i).start()
    for i in range(features // size):
        ship(i).wait()
    keep_att.wait()
    keep_gq.wait()


def finish_weight(rows, grads, attended, grad_queries):
    dp, keys, columns = grads.shape
    features = rows.shape[3]
    lanes = columns // HEAD
    flat = (features * lanes * 2, HEAD)
    weight, attended, grad_queries = pl.pallas_call(
        weight_kernel,
        in_specs=[VMEM, VMEM, VMEM, VMEM],
        out_specs=[ANY, ANY, ANY],
        out_shape=[
            jax.ShapeDtypeStruct(flat, jnp.float32),
            jax.ShapeDtypeStruct(attended.shape, attended.dtype),
            jax.ShapeDtypeStruct(attended.shape, attended.dtype),
        ],
        scratch_shapes=[pltpu.VMEM(flat, jnp.float32), DMA((2 + features // HEAD,))],
        compiler_params=pltpu.CompilerParams(vmem_limit_bytes=24 << 20),
        name="finish_weight",
    )(rows, grads, attended, grad_queries)
    weight = weight.reshape(features, lanes, 2, HEAD).transpose(0, 2, 1, 3).reshape(features, 2, columns)
    return attended, grad_queries, weight


def per_device(dp, ctx, text, src, lengths, kv_weight, queries, grad_out):
    chosen, rows, pair = gather_text(src, text[0], kv_weight, dp, ctx)
    dims = "ejtf,fec->ejtc"
    pair = pair.reshape((-1,) + kv_weight.shape[1:])
    part = jnp.einsum(dims, chosen, pair, preferred_element_type=jnp.float32)
    attended, grad_queries, grads = sublayer(src, lengths.T, part, queries[0], grad_out[0], dp, ctx)
    attended, grad_queries, weight = finish_weight(rows, grads, attended, grad_queries)
    return (attended[None], grad_queries[None], weight)


def solution(mesh):
    placed = (
        P("dp", None, None, "ctx"),
        P(),
        P(),
        P("dp", None, "ctx"),
        P("dp", "ctx", None),
        P("dp", "ctx", None),
    )
    return jax.shard_map(
        functools.partial(per_device, mesh.shape["dp"], mesh.shape["ctx"]),
        mesh=mesh,
        in_specs=placed,
        out_specs=(P("dp", "ctx", None), P("dp", "ctx", None), P("dp", None, "ctx")),
        check_vma=False,
    )
```

```python
import functools
import math

import jax
import jax.numpy as jnp
from jax import lax
from jax.experimental import pallas as pl
from jax.experimental.pallas import tpu as pltpu
from jax.sharding import PartitionSpec as P

HEAD = 128
PAIR = 2 * HEAD
STEP = 32
MESH = pl.DeviceIdType.MESH
VMEM = pl.BlockSpec(memory_space=pltpu.VMEM)
SMEM = pl.BlockSpec(memory_space=pltpu.SMEM)
ANY = pl.BlockSpec(memory_space=pl.ANY)
HBM = pl.BlockSpec(memory_space=pltpu.HBM)
DMA = pltpu.SemaphoreType.DMA


def dot(a, b, dims):
    return lax.dot_general(a, b, (dims, ((), ())), preferred_element_type=jnp.float32)


def remote(src, dst, send_sem, recv_sem, target):
    return pltpu.make_async_remote_copy(
        src_ref=src, dst_ref=dst, send_sem=send_sem, recv_sem=recv_sem, device_id=target, device_id_type=MESH
    )


class Place:
    def __init__(self, dp, ctx):
        self.rows, self.planes = dp // 2, ctx // 2
        self.last = self.planes - 1
        self.d, self.c = lax.axis_index("dp"), lax.axis_index("ctx")
        self.row, self.core = self.d // 2, self.d % 2
        self.a, self.b = self.c // 2, self.c % 2
        self.up = {"ctx": self.c + 2}
        self.down = {"ctx": self.c - 2}
        self.side = {"ctx": self.a * 2 + 1 - self.b}
        self.twin = {"dp": self.row * 2 + 1 - self.core}

    def at_row(self, row):
        return {"dp": row * 2 + self.core}

    def greet(self):
        barrier = pltpu.get_barrier_semaphore()

        def hello(target):
            pl.semaphore_signal(barrier, inc=1, device_id=target, device_id_type=MESH)

        hello(self.side)
        hello(self.twin)
        for j in range(self.rows):

            @pl.when(self.row != j)
            def _():
                hello(self.at_row(j))

        @pl.when(self.a < self.last)
        def _():
            hello(self.up)

        @pl.when(self.a > 0)
        def _():
            hello(self.down)

        fixed = 1 + self.rows
        if self.last == 0:
            pl.semaphore_wait(barrier, fixed)
        else:

            @pl.when((self.a > 0) & (self.a < self.last))
            def _():
                pl.semaphore_wait(barrier, fixed + 2)

            @pl.when((self.a == 0) | (self.a == self.last))
            def _():
                pl.semaphore_wait(barrier, fixed + 1)


def text_kernel(dp, ctx, src_any, own_ref, weight_ref, chosen_ref, text, pair_ref, src_ref, passing,
                src_sem, w_sems, line_send, line_recv, row_send, row_recv, side_send, side_recv,
                twin_send, twin_recv, copy_sems):
    me = Place(dp, ctx)
    rows, planes, a, b, last = me.rows, me.planes, me.a, me.b, me.last
    share = ctx // dp
    width = own_ref.shape[2]
    load_src = pltpu.make_async_copy(src_any, src_ref, src_sem)
    load_src.start()
    own_weights = pltpu.make_async_copy(weight_ref, pair_ref.at[0], w_sems.at[2])
    weights = remote(weight_ref, pair_ref.at[1], w_sems.at[0], w_sems.at[1], me.twin)
    me.greet()

    def slot(j, e, piece, core):
        at = (piece + core * share) % (2 * share) * width
        return text.at[e, j * 2 + me.core, :, pl.ds(pl.multiple_of(at, width), width)]

    def line(source, z, e, way, target):
        return remote(source, passing.at[z, e], line_send.at[z, e, way], line_recv.at[z, e], target)

    def to_row(source, z, e, j):
        row, i = z // share, z % share
        return remote(source, slot(j, e, i * 2 + b, me.core), row_send.at[z, e], row_recv.at[i, j, e], me.at_row(row))

    def to_side(source, i, j, e):
        return remote(source, slot(j, e, i * 2 + b, me.core), side_send.at[i, j, e], side_recv.at[i, j, e], me.side)

    def to_twin(source, piece, j, e):
        return remote(source, slot(j, e, piece, 1 - me.core), twin_send.at[piece, j, e],
                      twin_recv.at[piece, j, e], me.twin)

    def keep(source, i, e):
        return pltpu.make_async_copy(source, slot(me.row, e, i * 2 + b, me.core), copy_sems.at[i, e])

    def deliver(source, z, e):
        i = z % share

        @pl.when(z // share == me.row)
        def _():
            to_side(source, i, me.row, e).start()
            to_twin(source, i * 2 + b, me.row, e).start()
            keep(source, i, e).start()

        @pl.when(z // share != me.row)
        def _():
            to_row(source, z, e, me.row).start()

    def at_distance(s, body):
        for way in (0, 1) if s else (0,):
            z = a + s * (2 * way - 1)

            @pl.when((z >= 0) & (z <= last))
            def _():
                body(z, 1 - way)

    def arrive(z, way):
        target = me.up if way == 1 else me.down
        more = (a < last) if way == 1 else (a > 0)
        for e in range(2):
            source = passing.at[z, e]
            line(source, z, e, 0, me.up).wait_recv()

            @pl.when(more)
            def _():
                line(source, z, e, 1 - way, target).start()

            deliver(source, z, e)

    def from_rows(z, way):
        i = z % share

        @pl.when(z // share == me.row)
        def _():
            for j in range(rows):

                @pl.when(me.row != j)
                def _():
                    for e in range(2):
                        source = slot(j, e, i * 2 + b, me.core)
                        to_row(source, z, e, j).wait_recv()
                        to_side(source, i, j, e).start()
                        to_twin(source, i * 2 + b, j, e).start()

    def from_side(z, way):
        i = z % share

        @pl.when(z // share == me.row)
        def _():
            for j_at in range(rows):
                j = (me.row + j_at) % rows
                for e in range(2):
                    to_side(own_ref.at[e], i, j, e).wait_recv()
                    piece = i * 2 + 1 - b
                    to_twin(slot(j, e, piece, me.core), piece, j, e).start()

    for e in range(2):
        source = own_ref.at[e]

        @pl.when(a < last)
        def _():
            line(source, a, e, 0, me.up).start()

        @pl.when(a > 0)
        def _():
            line(source, a, e, 1, me.down).start()

        deliver(source, a, e)
    weights.start()
    own_weights.start()
    for s in range(1, planes + 2):
        if s < planes:
            at_distance(s, arrive)
        if s <= planes:
            at_distance(s - 1, from_rows)
        if s >= 2:
            at_distance(s - 2, from_side)

    load_src.wait()
    for i in range(share):
        for e in range(2):
            keep(own_ref.at[e], i, e).wait()
    for piece in range(2 * share):
        for j in range(rows):
            for e in range(2):
                to_twin(own_ref.at[e], piece, j, e).wait_recv()
    for e in range(2):
        for j in range(rows):
            chosen_ref[e, j] = text[e, src_ref[j * 2 + me.core]]
    weights.wait()
    own_weights.wait()
    for e in range(2):
        for piece in range(2 * share):
            for j in range(rows):
                to_twin(own_ref.at[e], piece, j, e).wait_send()
        for i in range(share):
            for j in range(rows):
                to_side(own_ref.at[e], i, j, e).wait_send()
        for z in range(planes):

            @pl.when(z // share != me.row)
            def _():
                to_row(own_ref.at[e], z, e, me.row).wait_send()

            @pl.when((a < last) & (z <= a))
            def _():
                line(own_ref.at[e], z, e, 0, me.up).wait_send()

            @pl.when((a > 0) & (z >= a))
            def _():
                line(own_ref.at[e], z, e, 1, me.down).wait_send()


def gather_text(src, own, weight, dp, ctx):
    tokens, width = own.shape[1:]
    share = ctx // dp
    rows = dp // 2
    kind = own.dtype
    pieces = 2 * share
    planes = ctx // 2
    return pl.pallas_call(
        functools.partial(text_kernel, dp, ctx),
        in_specs=[HBM, HBM, HBM],
        out_specs=[VMEM, VMEM, VMEM],
        out_shape=[
            jax.ShapeDtypeStruct((2, rows, tokens, pieces * width), kind),
            jax.ShapeDtypeStruct((2, dp, tokens, pieces * width), kind),
            jax.ShapeDtypeStruct((2,) + weight.shape, weight.dtype),
        ],
        scratch_shapes=[
            pltpu.SMEM(src.shape, src.dtype),
            pltpu.VMEM((planes, 2, tokens, width), kind),
            DMA,
            DMA((3,)),
            DMA((planes, 2, 2)),
            DMA((planes, 2)),
            DMA((planes, 2)),
            DMA((share, rows, 2)),
            DMA((share, rows, 2)),
            DMA((share, rows, 2)),
            DMA((pieces, rows, 2)),
            DMA((pieces, rows, 2)),
            DMA((share, 2)),
        ],
        compiler_params=pltpu.CompilerParams(collective_id=1, has_side_effects=True, vmem_limit_bytes=16 << 20),
        name="gather_text",
    )(src, own, weight)


def sublayer_kernel(dp, ctx, cut, src_any, lengths_any, part_ref, q_any, g_any, out_ref, gq_ref, grads_ref,
                    src_ref, lengths_ref, q_ref, g_ref, sums, kv, gkv, crossed0, risen0, fallen0, going0,
                    risen1, fallen1, going1, crossed1,
                    in_sems, y_send, y_recv, ag_send, ag_recv, x0_send, x0_recv,
                    up0_send, up0_recv, down0_send, down0_recv,
                    up1_send, up1_recv, down1_send, down1_recv, x1_send, x1_recv,
                    dp_send, dp_recv, twin_send):
    me = Place(dp, ctx)
    nrows, a, b, last = me.rows, me.a, me.b, me.last
    planes = me.planes
    rounds = kv.shape[0]
    keys = kv.shape[2]
    tokens = keys // 2
    own = me.c
    load_q = pltpu.make_async_copy(q_any, q_ref, in_sems.at[0])
    load_g = pltpu.make_async_copy(g_any, g_ref, in_sems.at[1])
    load_src = pltpu.make_async_copy(src_any, src_ref, in_sems.at[2])
    load_lengths = pltpu.make_async_copy(lengths_any, lengths_ref, in_sems.at[3])
    load_src.start()
    load_lengths.start()
    load_q.start()
    load_g.start()
    me.greet()
    parts = (pl.ds(0, cut), pl.ds(cut, keys - cut))
    pieces = ((1, cut - tokens, tokens), (0, 0, tokens), (1, 0, cut - tokens))

    def columns(r):
        return pl.ds(pl.multiple_of(r * PAIR, PAIR), PAIR)

    def partial(r, row, sender, piece):
        e, low, high = pieces[piece]
        return remote(part_ref.at[e, row, low:high, columns(r)], sums.at[r, sender, e, low:high, :],
                      y_send.at[r, row, piece], y_recv.at[r, sender, piece], me.at_row(row))

    def total(r, piece):
        e, low, high = pieces[piece]
        for j in range(nrows):

            @pl.when(me.row != j)
            def _():
                partial(r, j, j, piece).wait_recv()

        value = part_ref[e, me.row, low:high, columns(r)]
        for j_at in range(1, nrows):
            value = value + sums[r, (me.row + j_at) % nrows, e, low:high, :]
        kv[r, own, e * tokens + low:e * tokens + high, :] = value.astype(kv.dtype)

    def ag(r, part, block, way, target):
        where = kv.at[r, block, parts[part], :]
        return remote(where, where, ag_send.at[r, part, block, way], ag_recv.at[r, part, block], target)

    def ag_wait(r, part, block):
        ag(r, part, block, 2, me.side).wait_recv()

    def send_up(r, part, block):
        @pl.when(a < last)
        def _():
            ag(r, part, block, 0, me.up).start()

    def send_down(r, part, block):
        @pl.when(a > 0)
        def _():
            ag(r, part, block, 1, me.down).start()

    def start_round(r, early=False):
        total(r, 0)
        ag(r, 1, own, 2, me.side).start()
        if early:
            send_up(r, 1, own)
            send_down(r, 1, own)
        total(r, 1)
        total(r, 2)
        send_up(r, 0, own)
        send_down(r, 0, own)
        ag(r, 0, own, 2, me.side).start()
        if not early:
            send_up(r, 1, own)
            send_down(r, 1, own)

    def relay_side(r):
        block = a * 2 + 1 - b
        ag_wait(r, 1, block)
        send_up(r, 1, block)
        send_down(r, 1, block)

    def relay(r, base, send, unit):
        side = b if unit < 2 else 1 - b
        part = 0 if unit == 0 else 1
        ag_wait(r, part, base + side)
        send(r, part, base + side)
        if part == 0:
            ag(r, 0, base + side, 2, me.side).start()

    scale = 1.0 / math.sqrt(HEAD)
    position = lax.broadcasted_iota(jnp.int32, (1, keys), 1)
    load_src.wait()
    load_lengths.wait()
    text_at = src_ref[me.d]
    bound = jnp.where(position < tokens, lengths_ref[0, text_at], lengths_ref[1, text_at] + tokens)
    bias = jnp.where(position < bound, 0.0, -1e30).astype(jnp.float32)

    def attend(r, block):
        at = pl.ds(pl.multiple_of((block * rounds + r) * HEAD, HEAD), HEAD)
        q = q_ref[:, at]
        g = g_ref[:, at]
        key = kv[r, block, :, :HEAD]
        value = kv[r, block, :, HEAD:]
        scores = dot(q, key, ((1,), (1,))) * scale + bias
        grad_probs = dot(g, value, ((1,), (1,)))
        top = jnp.max(scores, axis=-1, keepdims=True)
        weights = jnp.exp(scores - top)
        probs = weights * (1.0 / jnp.sum(weights, axis=-1, keepdims=True))
        probs_low = probs.astype(jnp.bfloat16)
        delta = jnp.sum(probs * grad_probs, axis=-1, keepdims=True)
        grad_scores = (probs * (grad_probs - delta) * scale).astype(jnp.bfloat16)
        out_ref[:, at] = dot(probs_low, value, ((1,), (0,))).astype(jnp.bfloat16)
        gq_ref[:, at] = dot(grad_scores, key, ((1,), (0,))).astype(jnp.bfloat16)
        gkv[r, block, :, :HEAD] = dot(grad_scores, q, ((0,), (0,))).astype(gkv.dtype)
        gkv[r, block, :, HEAD:] = dot(probs_low, g, ((0,), (0,))).astype(gkv.dtype)

    def cross0(r, z):
        return remote(gkv.at[r, z * 2 + 1 - b, parts[0], :], crossed0.at[r, z], x0_send.at[r, z],
                      x0_recv.at[r, z], me.side)

    def work(r, s):
        @pl.loop(0, 4)
        def _(t):
            way, foreign = t // 2, t % 2
            far = s - foreign
            z = a + far * (2 * way - 1)
            block = z * 2 + b + foreign * (1 - 2 * b)

            @pl.when((z >= 0) & (z <= last) & (far >= 0) & (far <= last) & ((far > 0) | (way == 0)))
            def _():
                @pl.when(foreign == 1)
                def _():
                    ag_wait(r, 0, block)

                attend(r, block)

                @pl.when(foreign == 1)
                def _():
                    cross0(r, z).start()

    def chain0(r, z, rising):
        if rising:
            return remote(going0.at[r, z], risen0.at[r, z], up0_send.at[r, z], up0_recv.at[r, z], me.up)
        return remote(going0.at[r, z], fallen0.at[r, z], down0_send.at[r, z], down0_recv.at[r, z], me.down)

    def chain1(r, z, side, rising, source):
        if rising:
            return remote(source, risen1.at[r, z, side], up1_send.at[r, z, side], up1_recv.at[r, z, side], me.up)
        return remote(source, fallen1.at[r, z, side], down1_send.at[r, z, side], down1_recv.at[r, z, side], me.down)

    def add(target, terms):
        @pl.loop(0, target.shape[0] // STEP)
        def _(i):
            at = pl.ds(pl.multiple_of(i * STEP, STEP), STEP)
            total = terms[0][at, :].astype(jnp.float32)
            for term in terms[1:]:
                total = total + term[at, :].astype(jnp.float32)
            target[at, :] = total.astype(target.dtype)

    def pass_on(r, z, rising, begins, unit):
        arrived0 = risen0 if rising else fallen0
        arrived1 = risen1 if rising else fallen1
        if unit < 2:
            side = b if unit == 0 else 1 - b
            source = gkv.at[r, z * 2 + side, parts[1], :]
            if not begins:
                target = going1.at[r, z, side]
                chain1(r, z, side, rising, target).wait_recv()
                add(target, [source, arrived1.at[r, z, side]])
                source = target
            chain1(r, z, side, rising, source).start()
        else:
            cross0(r, z).wait_recv()
            terms = [gkv.at[r, z * 2 + b, parts[0], :], crossed0.at[r, z]]
            if not begins:
                chain0(r, z, rising).wait_recv()
                terms.append(arrived0.at[r, z])
            add(going0.at[r, z], terms)
            chain0(r, z, rising).start()

    def move(i, s, unit):
        @pl.when((i < rounds) & (a >= s))
        def _():
            relay(i, (a - s) * 2, send_up, unit)

        @pl.when((i > 0) & (a == 0))
        def _():
            pass_on(i - 1, last + 1 - s, True, True, unit)

        @pl.when((i > 0) & (a > 0) & (a < s))
        def _():
            pass_on(i - 1, last + a + 1 - s, True, False, unit)

        @pl.when((i < rounds) & (a + s <= last))
        def _():
            relay(i, (a + s) * 2, send_down, unit)

        @pl.when((i > 0) & (a == last))
        def _():
            pass_on(i - 1, s - 1, False, True, unit)

        @pl.when((i > 0) & (a < last) & (last - a < s))
        def _():
            pass_on(i - 1, s - last + a - 1, False, False, unit)

    def own_terms(r, low, high, side=None):
        terms = []
        if side is None:
            terms += [risen0.at[r, a]] * low + [fallen0.at[r, a]] * high
        else:
            terms += [risen1.at[r, a, side]] * low + [fallen1.at[r, a, side]] * high
        return terms

    def cross1(r):
        return remote(going1.at[r, a, 1 - b], crossed1.at[r], x1_send.at[r], x1_recv.at[r], me.side)

    def by_place(body):
        @pl.when(a == 0)
        def _():
            body(0, 1)

        @pl.when(a == last)
        def _():
            body(1, 0)

        @pl.when((a > 0) & (a < last))
        def _():
            body(1, 1)

    def finish(r):
        def body(low, high):
            for rising in (True,) * low + (False,) * high:
                for side in range(2):
                    chain1(r, a, side, rising, going1.at[r, a, side]).wait_recv()
            add(going1.at[r, a, 1 - b],
                [gkv.at[r, a * 2 + 1 - b, parts[1], :]] + own_terms(r, low, high, 1 - b))
            cross1(r).start()
            for rising in (True,) * low + (False,) * high:
                chain0(r, a, rising).wait_recv()
            cross0(r, a).wait_recv()
            add(grads_ref.at[me.d, parts[0], columns(r)],
                [gkv.at[r, own, parts[0], :], crossed0.at[r, a]] + own_terms(r, low, high))

        by_place(body)
        publish(r, 0)

    def share_grads(r, part, d, way, target):
        where = grads_ref.at[d, parts[part], columns(r)]
        return remote(where, where, dp_send.at[r, part, way], dp_recv.at[r, part, d], target)

    def hand_over(r, part, d):
        where = grads_ref.at[d, parts[part], columns(r)]
        return remote(where, where, twin_send.at[r, part, d // 2], dp_recv.at[r, part, d], me.twin)

    def publish(r, part):
        for j in range(nrows):

            @pl.when(me.row != j)
            def _():
                share_grads(r, part, me.d, j, me.at_row(j)).start()

        hand_over(r, part, me.d).start()

    def close(r):
        cross1(r).wait_recv()

        def body(low, high):
            add(grads_ref.at[me.d, parts[1], columns(r)],
                [gkv.at[r, own, parts[1], :], crossed1.at[r]] + own_terms(r, low, high, b))

        by_place(body)
        publish(r, 1)

    def spread(r):
        for part in range(2):
            for j in range(nrows):

                @pl.when(me.row != j)
                def _():
                    d = j * 2 + me.core
                    share_grads(r, part, d, j, me.at_row(j)).wait_recv()
                    hand_over(r, part, d).start()

    @pl.loop(0, rounds)
    def _(r):
        for j in range(nrows):

            @pl.when(me.row != j)
            def _():
                for piece in range(3):
                    partial(r, j, me.row, piece).start()

    start_round(0, True)
    load_q.wait()
    load_g.wait()

    @pl.loop(0, rounds + 1)
    def _(i):
        for s in range(planes):

            if s == 0:

                @pl.when(i < rounds)
                def _():
                    relay_side(i)

            else:
                for unit in range(3):
                    move(i, s, unit)

            if s == last:

                @pl.when(i + 1 < rounds)
                def _():
                    start_round(i + 1)

            if s == min(1, last):

                @pl.when(i > 1)
                def _():
                    finish(i - 2)

            if s == min(2, last):

                @pl.when(i > 1)
                def _():
                    close(i - 2)

            if s == last:

                @pl.when(i > 2)
                def _():
                    spread(i - 3)

            @pl.when(i < rounds)
            def _():
                work(i, s)

        @pl.when(i < rounds)
        def _():
            work(i, planes)

    finish(rounds - 1)
    close(rounds - 1)
    for r in range(max(rounds - 2, 0), rounds):
        spread(r)

    @pl.loop(0, rounds)
    def _(r):
        for j in range(nrows):
            for part in range(2):
                hand_over(r, part, j * 2 + 1 - me.core).wait_recv()
                hand_over(r, part, j * 2 + me.core).wait_send()

            @pl.when(me.row != j)
            def _():
                for piece in range(3):
                    partial(r, j, me.row, piece).wait_send()
                for part in range(2):
                    share_grads(r, part, me.d, j, me.at_row(j)).wait_send()

        ag(r, 1, own, 2, me.side).wait_send()
        cross1(r).wait_send()
        for z in range(planes):
            cross0(r, z).wait_send()
            ag(r, 0, z * 2 + b, 2, me.side).wait_send()

            @pl.when((a < last) & (z <= a))
            def _():
                ag(r, 0, z * 2 + b, 0, me.up).wait_send()
                for side in range(2):
                    ag(r, 1, z * 2 + side, 0, me.up).wait_send()

            @pl.when((a > 0) & (z >= a))
            def _():
                ag(r, 0, z * 2 + b, 1, me.down).wait_send()
                for side in range(2):
                    ag(r, 1, z * 2 + side, 1, me.down).wait_send()

            for rising in (True, False):

                @pl.when((z > a) if rising else (z < a))
                def _():
                    chain0(r, z, rising).wait_send()
                    for side in range(2):
                        chain1(r, z, side, rising, going1.at[r, z, side]).wait_send()


def sublayer(src, lengths, part, queries, grad_out, dp, ctx):
    _, rows, tokens, columns = part.shape
    rounds = columns // PAIR
    keys = 2 * tokens
    planes = ctx // 2
    cut = keys * 5 // 8 // STEP * STEP
    low = jnp.bfloat16
    first = pltpu.VMEM((rounds, planes, cut, PAIR), low)
    second = pltpu.VMEM((rounds, planes, 2, keys - cut, PAIR), low)
    whole = pltpu.VMEM((rounds, ctx, keys, PAIR), low)
    return pl.pallas_call(
        functools.partial(sublayer_kernel, dp, ctx, cut),
        in_specs=[HBM, HBM, VMEM, HBM, HBM],
        out_specs=[VMEM, VMEM, VMEM],
        out_shape=[
            jax.ShapeDtypeStruct(queries.shape, low),
            jax.ShapeDtypeStruct(queries.shape, low),
            jax.ShapeDtypeStruct((dp, keys, columns), low),
        ],
        scratch_shapes=[
            pltpu.SMEM(src.shape, src.dtype),
            pltpu.SMEM(lengths.shape, lengths.dtype),
            pltpu.VMEM(queries.shape, low),
            pltpu.VMEM(queries.shape, low),
            pltpu.VMEM((rounds, rows, 2, tokens, PAIR), jnp.float32),
            whole,
            whole,
            first,
            first,
            first,
            first,
            second,
            second,
            second,
            pltpu.VMEM((rounds, keys - cut, PAIR), low),
            DMA((4,)),
            DMA((rounds, rows, 3)),
            DMA((rounds, rows, 3)),
            DMA((rounds, 2, ctx, 3)),
            DMA((rounds, 2, ctx)),
        ]
        + [DMA((rounds, planes))] * 6
        + [DMA((rounds, planes, 2))] * 4
        + [
            DMA((rounds,)),
            DMA((rounds,)),
            DMA((rounds, 2, rows)),
            DMA((rounds, 2, dp)),
            DMA((rounds, 2, rows)),
        ],
        compiler_params=pltpu.CompilerParams(collective_id=2, has_side_effects=True, vmem_limit_bytes=44 << 20),
        name="sublayer",
    )(src, lengths, part, queries, grad_out)


def weight_kernel(src_ref, rows_ref, grads_ref, att_ref, gq_ref, out_ref, att_out, gq_out, buffer, sems):
    keep_att = pltpu.make_async_copy(att_ref, att_out, sems.at[0])
    keep_gq = pltpu.make_async_copy(gq_ref, gq_out, sems.at[1])
    keep_att.start()
    keep_gq.start()
    dp, keys, columns = grads_ref.shape
    tokens = keys // 2
    features = rows_ref.shape[3] // 2
    lanes = columns // HEAD
    stride = 2 * lanes
    size = HEAD

    def ship(i):
        at = pl.ds(i * size * stride, size * stride)
        return pltpu.make_async_copy(buffer.at[at, :], out_ref.at[at, :], sems.at[2 + i])

    for i in range(features // size):
        for e in range(2):
            left = jnp.concatenate(
                [rows_ref[e, src_ref[at], :, i * size:(i + 1) * size] for at in range(dp)], axis=0
            )
            for j in range(columns // PAIR):
                right = grads_ref[:, e * tokens:(e + 1) * tokens, j * PAIR:(j + 1) * PAIR].reshape(dp * tokens, PAIR)
                block = dot(left, right, ((0,), (0,)))
                for half in range(2):
                    buffer[pl.ds(i * size * stride + (2 * j + half) * 2 + e, size, stride), :] = (
                        block[:, half * HEAD:(half + 1) * HEAD]
                    )
        ship(i).start()
    for i in range(features // size):
        ship(i).wait()
    keep_att.wait()
    keep_gq.wait()


def finish_weight(src, rows, grads, attended, grad_queries):
    dp, keys, columns = grads.shape
    features = rows.shape[3] // 2
    lanes = columns // HEAD
    flat = (features * lanes * 2, HEAD)
    weight, attended, grad_queries = pl.pallas_call(
        weight_kernel,
        in_specs=[SMEM, VMEM, VMEM, VMEM, VMEM],
        out_specs=[ANY, ANY, ANY],
        out_shape=[
            jax.ShapeDtypeStruct(flat, jnp.float32),
            jax.ShapeDtypeStruct(attended.shape, attended.dtype),
            jax.ShapeDtypeStruct(attended.shape, attended.dtype),
        ],
        scratch_shapes=[pltpu.VMEM(flat, jnp.float32), DMA((2 + features // HEAD,))],
        compiler_params=pltpu.CompilerParams(vmem_limit_bytes=24 << 20),
        name="finish_weight",
    )(src, rows, grads, attended, grad_queries)
    weight = weight.reshape(features, lanes, 2, HEAD).transpose(0, 2, 1, 3).reshape(features, 2, columns)
    return attended, grad_queries, weight


def per_device(dp, ctx, text, src, lengths, kv_weight, queries, grad_out):
    chosen, rows, pair = gather_text(src, text[0], kv_weight, dp, ctx)
    dims = "ejtf,fec->ejtc"
    pair = pair.reshape((-1,) + kv_weight.shape[1:])
    part = jnp.einsum(dims, chosen, pair, preferred_element_type=jnp.float32)
    attended, grad_queries, grads = sublayer(src, lengths.T, part, queries[0], grad_out[0], dp, ctx)
    attended, grad_queries, weight = finish_weight(src, rows, grads, attended, grad_queries)
    return (attended[None], grad_queries[None], weight)


def solution(mesh):
    placed = (
        P("dp", None, None, "ctx"),
        P(),
        P(),
        P("dp", None, "ctx"),
        P("dp", "ctx", None),
        P("dp", "ctx", None),
    )
    return jax.shard_map(
        functools.partial(per_device, mesh.shape["dp"], mesh.shape["ctx"]),
        mesh=mesh,
        in_specs=placed,
        out_specs=(P("dp", "ctx", None), P("dp", "ctx", None), P("dp", None, "ctx")),
        check_vma=False,
    )
```
